128 devices in a mesh: dp: 32 (over z, y, x_hi), tensor: 4 (over x_lo, core).
Axes of the slice: x: 4 (x_hi: 2, x_lo: 2; x = x_hi * 2 + x_lo), y: 4, z: 4, core: 2. Of those that a mesh axis runs over, the one named last changes fastest.
Arguments:
- hidden: bfloat16 [4096, 7168], P('dp', 'tensor'), may hold values from -6 to 6
- hash_rows: int32 [4096, 4], P('dp', 'tensor'), may hold values from 0 to 32767, as said below
- memory_table: bfloat16 [32768, 896], P(('dp', 'tensor')), may hold values from -6 to 6
- key_weight: bfloat16 [3584, 7168], P(None, 'tensor'), may hold values from -0.09375 to 0.09375
- value_weight: bfloat16 [3584, 7168], P(None, 'tensor'), may hold values from -0.09375 to 0.09375
- hidden_gain: float32 [7168], P('tensor'), may hold values from 0.1 to 1.9
- key_gain: float32 [7168], P('tensor'), may hold values from 0.1 to 1.9
Outputs:
- joined: bfloat16 [4096, 7168], P('dp', 'tensor')
The draws below stay inside these ranges and needn't reach their ends.
Inputs may be any that keep to these rules, and one draw needn't show every extreme that they name: `hash_rows`: row r lies in the block of 256 rows held by device r // 256 of dp+tensor. Of the lookups that one device holds (128 requests of its dp group times its 4 / 4 heads), at most 2 fall into any one device's block, and in every draw some device's block receives exactly 2 from every device.
All inputs are finite; a program needn't handle non-finite values.
Results may differ from the reference program's by a relative error of at most 0.0014.
Values may be sent and summed in bfloat16 or wider, within the bound.
No kernel may reach another device: no remote copies, remote signals or barrier semaphores. Data moves between devices by JAX's collectives and lax.ppermute only.
A program may use at most 64 MiB of HBM per device.

```python
import jax
import jax.numpy as jnp
from jax import lax

D = 7168
HEADW = 896
HEADS = 4
REQ = 128
ROWS_DEV = 256
MEM = 3584
TOKENS = 4096
ROWS = 32768
CAP = 2
N_DP = 32
N_TENSOR = 4


def draw_hash_rows(key, part):
    owners = N_DP * N_TENSOR
    per_device = REQ * (HEADS // N_TENSOR)
    slot_count = owners * CAP
    hot_owner = jax.random.randint(jax.random.fold_in(key, 11), (), 0, owners)
    slot_owner = jnp.arange(slot_count, dtype=jnp.int32) // CAP
    slot_rank = jnp.arange(slot_count, dtype=jnp.int32) % CAP

    def one_device(device_index):
        device_key = jax.random.fold_in(jax.random.fold_in(key, 23), device_index)
        shuffle_order = jax.random.permutation(jax.random.fold_in(device_key, 1), slot_count)
        placing = jnp.zeros((slot_count,), jnp.int32).at[shuffle_order].set(jnp.arange(slot_count, dtype=jnp.int32))
        priority = jnp.where(slot_owner == hot_owner, slot_rank - CAP, placing)
        chosen = jnp.argsort(priority, stable=True)[:per_device]
        picked = slot_owner[chosen]
        shuffled = picked[jax.random.permutation(jax.random.fold_in(device_key, 2), per_device)]
        local_rows = jax.random.randint(jax.random.fold_in(device_key, 3), (per_device,), 0, ROWS_DEV)
        return shuffled * ROWS_DEV + local_rows
    drawn = jax.vmap(one_device)(jnp.arange(owners, dtype=jnp.int32))
    blocks = drawn.reshape(N_DP, N_TENSOR, REQ, HEADS // N_TENSOR)
    return jnp.transpose(blocks, (0, 2, 1, 3)).reshape(N_DP * REQ, HEADS).astype(jnp.int32)


def block_levels(rng, dims, split, least, largest):
    loudness, own = 1.0, jax.random.fold_in(rng, 6)
    for dim, blocks in split:
        draws = jnp.exp(jax.random.uniform(jax.random.fold_in(own, dim), (blocks,), jnp.float32, least / len(split), largest / len(split)))
        loudness = loudness * jnp.repeat(draws, dims[dim] // blocks).reshape([-1 if axis == dim else 1 for axis in range(len(dims))])
    return loudness


def gaussian(stream_key, extent, scale, bound, cuts=(), kind=jnp.bfloat16):
    entries = jax.random.normal(stream_key, extent, jnp.float32) * scale
    if len(cuts) > 0:
        entries = block_levels(stream_key, extent, cuts, -0.22, 0.18) * entries
    return jnp.clip(entries, min=-bound, max=bound).astype(kind)


def setup_inputs(seed: int = 0) -> dict:
    key_of = jax.random.split(jax.random.key(seed), 8)
    hidden = gaussian(key_of[0], (TOKENS, D), 1.0, 6.0, ((0, 32), (1, 4)))
    hash_rows = draw_hash_rows(jax.random.fold_in(key_of[7], 71), 0)
    memory_table = gaussian(key_of[2], (ROWS, HEADW), 1.0, 6.0, ((0, 128),))
    key_weight = gaussian(key_of[3], (MEM, D), MEM ** -0.5, 0.09375, ((1, 4),))
    value_weight = gaussian(key_of[4], (MEM, D), MEM ** -0.5, 0.09375, ((1, 4),))
    hidden_gain = jnp.clip(1.0 + 0.18 * jax.random.normal(key_of[5], (D,), jnp.float32), 0.1, 1.9)
    key_gain = jnp.clip(1.0 + 0.18 * jax.random.normal(key_of[6], (D,), jnp.float32), 0.1, 1.9)
    return {"hidden": hidden, "hash_rows": hash_rows, "memory_table": memory_table, "key_weight": key_weight, "value_weight": value_weight, "hidden_gain": hidden_gain, "key_gain": key_gain}


epsilon = 1e-06

def reference(hidden, hash_rows, memory_table, key_weight, value_weight, hidden_gain, key_gain):

    def group_output(arrays):
        hidden_rows, index_rows = arrays
        memory = memory_table[index_rows].reshape(index_rows.shape[0], MEM)
        key = jnp.dot(memory, key_weight, preferred_element_type=jnp.float32)
        projected = jnp.dot(memory, value_weight, preferred_element_type=jnp.float32)
        hidden_float = hidden_rows.astype(jnp.float32)
        hidden_power = lax.optimization_barrier(jnp.mean(hidden_float * hidden_float, axis=1))
        key_power = lax.optimization_barrier(jnp.mean(key * key, axis=1))
        crossing = lax.optimization_barrier(jnp.sum(hidden_float * hidden_gain * key * key_gain, axis=1))
        agreement = crossing * lax.rsqrt(hidden_power + epsilon) * lax.rsqrt(key_power + epsilon)
        gate_value = jax.nn.sigmoid(agreement / jnp.sqrt(jnp.float32(D)))
        return (hidden_float + gate_value[:, None] * projected).astype(jnp.bfloat16)
    outputs = lax.map(group_output, (hidden.reshape(N_DP, REQ, D), hash_rows.reshape(N_DP, REQ, HEADS)))
    return outputs.reshape(N_DP * REQ, D)
```

```python
import math

import jax
import jax.numpy as jnp
from jax import lax
from jax.experimental import pallas as pl
from jax.experimental.pallas import tpu as pltpu
from jax.sharding import PartitionSpec as P

D = 7168
LANES = 128
EPSILON = 1e-06
COVER = 20_000_000_000
BOTH = ("dp", "tensor")
MIB = 1024 * 1024

f32 = jnp.float32
bf16 = jnp.bfloat16


def iota(shape, dim):
    return lax.broadcasted_iota(jnp.int32, shape, dim)


def vmem(count):
    return [pl.BlockSpec(memory_space=pltpu.VMEM)] * count


def call(body, out_shape, inputs, limit, scalars=(), scratch=(), flops=0):
    many = isinstance(out_shape, (tuple, list))
    return pl.pallas_call(
        body,
        out_shape=out_shape,
        in_specs=[pl.BlockSpec(memory_space=pltpu.SMEM)] * len(scalars) + vmem(len(inputs)),
        out_specs=tuple(vmem(len(out_shape))) if many else vmem(1)[0],
        scratch_shapes=list(scratch),
        compiler_params=pltpu.CompilerParams(vmem_limit_bytes=limit),
        cost_estimate=pl.CostEstimate(flops=flops, transcendentals=0, bytes_accessed=0) if flops else None,
    )(*scalars, *inputs)


def request_kernel(rows_held, hash_ref, out_ref):
    row = hash_ref[...]
    owner = row // rows_held
    local = row - owner * rows_held
    owner_rows = jnp.broadcast_to(owner.astype(f32), (LANES, LANES))
    owner_cols = owner_rows.T
    earlier = (owner_rows == owner_cols) & (iota((LANES, LANES), 0) < iota((LANES, LANES), 1))
    slot = jnp.sum(earlier.astype(f32), axis=0, keepdims=True)
    position = owner * 2 + slot.astype(jnp.int32)
    place = iota((LANES, LANES), 0)
    local_f = local.astype(f32)
    zero = jnp.zeros((LANES, LANES), f32)
    ask0 = jnp.sum(jnp.where(position == 2 * place, local_f, zero), axis=1, keepdims=True)
    ask1 = jnp.sum(jnp.where(position == 2 * place + 1, local_f, zero), axis=1, keepdims=True)
    asks = jnp.where(iota((LANES, LANES), 1) < LANES // 2, ask0, ask1)
    where = jnp.broadcast_to(position.astype(f32), (LANES, LANES))
    both = jnp.stack([where, asks], axis=1)
    out_ref[...] = both.reshape(2 * LANES, LANES).astype(bf16)


def gather_kernel(asked_ref, table_ref, out_ref):
    asked = asked_ref[...].astype(f32)
    rows = asked.shape[0]
    even = (iota((rows, 1), 0) % 2) == 0
    ahead = pltpu.roll(asked, rows - 1, 0)
    index = jnp.where(even, ahead[:, 0:1], asked[:, LANES - 1 :])
    held = table_ref.shape[0]
    chosen = (index.astype(jnp.int32) == iota((rows, held), 1)).astype(f32).astype(bf16)
    found = jnp.dot(chosen, table_ref[...], preferred_element_type=f32)
    found = found.astype(bf16).reshape(rows // 8, 1, 8, found.shape[1])
    out_ref[...] = jnp.concatenate([found, found], axis=1).reshape(2 * rows, -1)


def place_kernel(where_ref, asked_ref, arrived_ref, out_ref):
    core = where_ref[0] & 1
    start = pl.multiple_of((where_ref[0] >> 2) * 8, 8)
    asked = asked_ref[pl.ds(start, 8), :].astype(f32)
    arrived = arrived_ref[...]
    slots = arrived.shape[0]
    width = arrived.shape[1]
    for head in range(4):
        position = jnp.broadcast_to(asked[2 * head : 2 * head + 1, :], (LANES, LANES)).T
        position = position[:, 0:1].astype(jnp.int32)
        owner = position // 2
        target = (owner // 2) * 8 + head * 2 + position % 2
        target = jnp.where(owner % 2 == core, target, -1)
        chosen = (target == iota((LANES, slots), 1)).astype(f32).astype(bf16)
        found = jnp.dot(chosen, arrived, preferred_element_type=f32)
        out_ref[:, head * width : (head + 1) * width] = found.astype(bf16)


def row_of_sums(terms):
    parts = terms[:, 0:LANES]
    for k in range(1, terms.shape[1] // LANES):
        parts = parts + terms[:, k * LANES : (k + 1) * LANES]
    return jnp.sum(parts.T, axis=0, keepdims=True)


def key_kernel(mine_ref, other_ref, weight_ref, hidden_ref, hgain_ref, kgain_ref, memory_ref, sums_ref):
    memory = mine_ref[...] + other_ref[...]
    memory_ref[...] = memory
    key = jnp.dot(memory, weight_ref[...], preferred_element_type=f32)
    hidden = hidden_ref[...].astype(f32)
    sums = [
        row_of_sums(hidden * hidden),
        row_of_sums(key * key),
        row_of_sums((hidden * hgain_ref[...]) * (key * kgain_ref[...])),
    ]
    sums_ref[...] = jnp.concatenate(sums + [jnp.zeros((5, LANES), f32)], axis=0)


def value_kernel(memory_ref, weight_ref, out_ref):
    out_ref[...] = jnp.dot(memory_ref[...], weight_ref[...], preferred_element_type=f32)


def join_kernel(s0_ref, s1_ref, s2_ref, s3_ref, hidden_ref, projected_ref, out_ref):
    sums = (s0_ref[...] + s1_ref[...]) + (s2_ref[...] + s3_ref[...])
    hidden_power = sums[0:1] / D
    key_power = sums[1:2] / D
    agreement = sums[2:3] * lax.rsqrt(hidden_power + EPSILON) * lax.rsqrt(key_power + EPSILON)
    gate = jax.nn.sigmoid(agreement / math.sqrt(D))
    gate = jnp.broadcast_to(gate, (LANES, LANES)).T[:, 0:1]
    out_ref[...] = (hidden_ref[...].astype(f32) + gate * projected_ref[...]).astype(bf16)


def local(hidden, hash_rows, memory_table, key_weight, value_weight, hidden_gain, key_gain):
    groups = lax.axis_size("dp")
    tensor = lax.axis_size("tensor")
    devices = groups * tensor
    rows_held, row_width = memory_table.shape
    shape = jax.ShapeDtypeStruct

    here = lax.axis_index(BOTH).astype(jnp.int32).reshape(1)
    hash_rows, here, hidden_gain, key_gain = lax.optimization_barrier((hash_rows, here, hidden_gain, key_gain))
    message = call(
        lambda *refs: request_kernel(rows_held, *refs),
        shape((2 * devices, LANES), bf16),
        [hash_rows.reshape(1, LANES)],
        4 * MIB,
        flops=COVER,
    )
    asked = lax.all_to_all(message.reshape(devices, 2, LANES), BOTH, 0, 0, tiled=True)
    asked = asked.reshape(2 * devices, LANES)
    sent = call(gather_kernel, shape((4 * devices, row_width), bf16), [asked, memory_table], 6 * MIB, flops=COVER)
    same_core = [[2 * k + c for k in range(devices // 2)] for c in range(2)]
    arrived = lax.all_to_all(
        sent.reshape(devices // 2, 8, row_width), BOTH, 0, 0, axis_index_groups=same_core, tiled=True
    ).reshape(4 * devices, row_width)
    mine = call(
        place_kernel,
        shape((LANES, 4 * row_width), bf16),
        [asked, arrived],
        6 * MIB,
        scalars=[here],
    )
    other = lax.ppermute(mine, "tensor", [(k, k ^ 1) for k in range(tensor)])
    columns = key_weight.shape[1]
    key_weight = pltpu.with_memory_space_constraint(key_weight, pltpu.VMEM)
    value_weight = pltpu.with_memory_space_constraint(value_weight, pltpu.VMEM)
    memory, sums = call(
        key_kernel,
        (shape(mine.shape, bf16), shape((8, LANES), f32)),
        [mine, other, key_weight, hidden, hidden_gain.reshape(1, columns), key_gain.reshape(1, columns)],
        6 * MIB,
        flops=2 * LANES * mine.shape[1] * columns,
    )
    others = [lax.ppermute(sums, "tensor", [(k, k ^ d) for k in range(tensor)]) for d in (1, 2, 3)]
    projected = call(
        value_kernel,
        shape((LANES, columns), f32),
        [memory, value_weight],
        6 * MIB,
        flops=2 * LANES * mine.shape[1] * columns,
    )
    return call(join_kernel, shape(hidden.shape, bf16), [sums, *others, hidden, projected], 6 * MIB)


def solution(mesh):
    return jax.shard_map(
        local,
        mesh=mesh,
        in_specs=(
            P("dp", "tensor"),
            P("dp", "tensor"),
            P(("dp", "tensor"), None),
            P(None, "tensor"),
            P(None, "tensor"),
            P("tensor"),
            P("tensor"),
        ),
        out_specs=P("dp", "tensor"),
        check_vma=False,
    )
```

```python
import math

import jax
import jax.numpy as jnp
from jax import lax
from jax.experimental import pallas as pl
from jax.experimental.pallas import tpu as pltpu
from jax.sharding import PartitionSpec as P

D = 7168
LANES = 128
EPSILON = 1e-06
COVER = 20_000_000_000
BOTH = ("dp", "tensor")
MIB = 1024 * 1024

f32 = jnp.float32
bf16 = jnp.bfloat16


def iota(shape, dim):
    return lax.broadcasted_iota(jnp.int32, shape, dim)


def vmem(count):
    return [pl.BlockSpec(memory_space=pltpu.VMEM)] * count


def call(body, out_shape, inputs, limit, scalars=(), scratch=(), flops=0):
    many = isinstance(out_shape, (tuple, list))
    return pl.pallas_call(
        body,
        out_shape=out_shape,
        in_specs=[pl.BlockSpec(memory_space=pltpu.SMEM)] * len(scalars) + vmem(len(inputs)),
        out_specs=tuple(vmem(len(out_shape))) if many else vmem(1)[0],
        scratch_shapes=list(scratch),
        compiler_params=pltpu.CompilerParams(vmem_limit_bytes=limit),
        cost_estimate=pl.CostEstimate(flops=flops, transcendentals=0, bytes_accessed=0) if flops else None,
    )(*scalars, *inputs)


def request_kernel(rows_held, hash_ref, out_ref):
    row = hash_ref[...]
    owner = row // rows_held
    local = row - owner * rows_held
    owner_rows = jnp.broadcast_to(owner.astype(f32), (LANES, LANES))
    owner_cols = owner_rows.T
    earlier = (owner_rows == owner_cols) & (iota((LANES, LANES), 0) < iota((LANES, LANES), 1))
    slot = jnp.sum(earlier.astype(f32), axis=0, keepdims=True)
    position = owner * 2 + slot.astype(jnp.int32)
    place = iota((LANES, LANES), 0)
    local_f = local.astype(f32)
    zero = jnp.zeros((LANES, LANES), f32)
    ask0 = jnp.sum(jnp.where(position == 2 * place, local_f, zero), axis=1, keepdims=True)
    ask1 = jnp.sum(jnp.where(position == 2 * place + 1, local_f, zero), axis=1, keepdims=True)
    asks = jnp.where(iota((LANES, LANES), 1) < LANES // 2, ask0, ask1)
    where = jnp.broadcast_to(position.astype(f32), (LANES, LANES))
    both = jnp.stack([where, asks], axis=1)
    out_ref[...] = both.reshape(2 * LANES, LANES).astype(bf16)


def gather_kernel(asked_ref, table_ref, out_ref):
    asked = asked_ref[...].astype(f32)
    rows = asked.shape[0]
    even = (iota((rows, 1), 0) % 2) == 0
    ahead = pltpu.roll(asked, rows - 1, 0)
    index = jnp.where(even, ahead[:, 0:1], asked[:, LANES - 1 :])
    held = table_ref.shape[0]
    chosen = (index.astype(jnp.int32) == iota((rows, held), 1)).astype(f32).astype(bf16)
    found = jnp.dot(chosen, table_ref[...], preferred_element_type=f32)
    found = found.astype(bf16).reshape(rows // 8, 1, 8, found.shape[1])
    out_ref[...] = jnp.concatenate([found, found], axis=1).reshape(2 * rows, -1)


def place_kernel(heads, where_ref, asked_ref, arrived_ref, out_ref):
    core = where_ref[0] & 1
    start = pl.multiple_of((where_ref[0] >> 2) * 8, 8)
    asked = asked_ref[pl.ds(start, 8), :].astype(f32)
    arrived = arrived_ref[...]
    slots = arrived.shape[0]
    width = arrived.shape[1]
    for k, head in enumerate(heads):
        position = jnp.broadcast_to(asked[2 * head : 2 * head + 1, :], (LANES, LANES)).T
        position = position[:, 0:1].astype(jnp.int32)
        target = (position >> 2) * 8 + head * 2 + (position & 1)
        target = jnp.where(((position >> 1) & 1) == core, target, -1)
        chosen = (target == iota((LANES, slots), 1)).astype(f32).astype(bf16)
        found = jnp.dot(chosen, arrived, preferred_element_type=f32)
        out_ref[:, k * width : (k + 1) * width] = found.astype(bf16)


def row_of_sums(terms):
    parts = terms[:, 0:LANES]
    for k in range(1, terms.shape[1] // LANES):
        parts = parts + terms[:, k * LANES : (k + 1) * LANES]
    return jnp.sum(parts.T, axis=0, keepdims=True)


def first_kernel(mine_ref, other_ref, key_weight_ref, value_weight_ref, key_ref, value_ref):
    memory = mine_ref[...] + other_ref[...]
    depth = memory.shape[1]
    key_ref[...] = jnp.dot(memory, key_weight_ref[:depth, :], preferred_element_type=f32)
    value_ref[...] = jnp.dot(memory, value_weight_ref[:depth, :], preferred_element_type=f32)


def key_kernel(mine_ref, other_ref, weight_ref, first_ref, hidden_ref, hgain_ref, kgain_ref, sums_ref):
    memory = mine_ref[...] + other_ref[...]
    depth = memory.shape[1]
    key = first_ref[...] + jnp.dot(memory, weight_ref[depth:, :], preferred_element_type=f32)
    hidden = hidden_ref[...].astype(f32)
    sums = [
        row_of_sums(hidden * hidden),
        row_of_sums(key * key),
        row_of_sums((hidden * hgain_ref[...]) * (key * kgain_ref[...])),
    ]
    sums_ref[...] = jnp.concatenate(sums + [jnp.zeros((5, LANES), f32)], axis=0)


def value_kernel(mine_ref, other_ref, weight_ref, first_ref, out_ref):
    memory = mine_ref[...] + other_ref[...]
    depth = memory.shape[1]
    out_ref[...] = first_ref[...] + jnp.dot(memory, weight_ref[depth:, :], preferred_element_type=f32)


def join_kernel(s0_ref, s1_ref, s2_ref, s3_ref, hidden_ref, projected_ref, out_ref):
    sums = (s0_ref[...] + s1_ref[...]) + (s2_ref[...] + s3_ref[...])
    hidden_power = sums[0:1] / D
    key_power = sums[1:2] / D
    agreement = sums[2:3] * lax.rsqrt(hidden_power + EPSILON) * lax.rsqrt(key_power + EPSILON)
    gate = jax.nn.sigmoid(agreement / math.sqrt(D))
    gate = jnp.broadcast_to(gate, (LANES, LANES)).T[:, 0:1]
    out_ref[...] = (hidden_ref[...].astype(f32) + gate * projected_ref[...]).astype(bf16)


def local(hidden, hash_rows, memory_table, key_weight, value_weight, hidden_gain, key_gain):
    groups = lax.axis_size("dp")
    tensor = lax.axis_size("tensor")
    devices = groups * tensor
    rows_held, row_width = memory_table.shape
    shape = jax.ShapeDtypeStruct

    here = lax.axis_index(BOTH).astype(jnp.int32).reshape(1)
    hash_rows, here, hidden_gain, key_gain = lax.optimization_barrier((hash_rows, here, hidden_gain, key_gain))
    message = call(
        lambda *refs: request_kernel(rows_held, *refs),
        shape((2 * devices, LANES), bf16),
        [hash_rows.reshape(1, LANES)],
        4 * MIB,
        flops=COVER,
    )
    asked = lax.all_to_all(message.reshape(devices, 2, LANES), BOTH, 0, 0, tiled=True)
    asked = asked.reshape(2 * devices, LANES)
    sent = call(gather_kernel, shape((4 * devices, row_width), bf16), [asked, memory_table], 6 * MIB, flops=COVER)
    same_core = [[2 * k + c for k in range(devices // 2)] for c in range(2)]
    arrived = lax.all_to_all(
        sent.reshape(devices // 2, 8, row_width), BOTH, 0, 0, axis_index_groups=same_core, tiled=True
    ).reshape(4 * devices, row_width)
    halves = []
    for heads in ((0, 1), (2, 3)):
        mine = call(
            lambda *refs, heads=heads: place_kernel(heads, *refs),
            shape((LANES, 2 * row_width), bf16),
            [asked, arrived],
            6 * MIB,
            scalars=[here],
        )
        halves.append((mine, lax.ppermute(mine, "tensor", [(k, k ^ 1) for k in range(tensor)])))
    columns = key_weight.shape[1]
    work = 2 * LANES * 2 * row_width * columns
    key_weight = pltpu.with_memory_space_constraint(key_weight, pltpu.VMEM)
    value_weight = pltpu.with_memory_space_constraint(value_weight, pltpu.VMEM)
    partial = shape((LANES, columns), f32)
    key, value = call(
        first_kernel, (partial, partial), [*halves[0], key_weight, value_weight], 6 * MIB, flops=2 * work
    )
    sums = call(
        key_kernel,
        shape((8, LANES), f32),
        [*halves[1], key_weight, key, hidden, hidden_gain.reshape(1, columns), key_gain.reshape(1, columns)],
        6 * MIB,
        flops=work,
    )
    others = [lax.ppermute(sums, "tensor", [(k, k ^ d) for k in range(tensor)]) for d in (1, 2, 3)]
    projected = call(value_kernel, partial, [*halves[1], value_weight, value], 6 * MIB, flops=work)
    return call(join_kernel, shape(hidden.shape, bf16), [sums, *others, hidden, projected], 6 * MIB)


def solution(mesh):
    return jax.shard_map(
        local,
        mesh=mesh,
        in_specs=(
            P("dp", "tensor"),
            P("dp", "tensor"),
            P(("dp", "tensor"), None),
            P(None, "tensor"),
            P(None, "tensor"),
            P("tensor"),
            P("tensor"),
        ),
        out_specs=P("dp", "tensor"),
        check_vma=False,
    )
```

```python
import math

import jax
import jax.numpy as jnp
from jax import lax
from jax.experimental import pallas as pl
from jax.experimental.pallas import tpu as pltpu
from jax.sharding import PartitionSpec as P

D = 7168
LANES = 128
EPSILON = 1e-06
COVER = 20_000_000_000
BOTH = ("dp", "tensor")
MIB = 1024 * 1024

f32 = jnp.float32
bf16 = jnp.bfloat16


def chip_order():
    order = []
    for k in range(64):
        a, b, c = k % 4, (k // 4) % 4, k // 16
        order.append(a * 16 + (a + b) % 4 * 4 + (a + b + c) % 4)
    return order


def turn_of(chip):
    z, y, x = chip >> 4, (chip >> 2) & 3, chip & 3
    return z + ((y - z) & 3) * 4 + ((x - y) & 3) * 16


def iota(shape, dim):
    return lax.broadcasted_iota(jnp.int32, shape, dim)


def vmem(count):
    return [pl.BlockSpec(memory_space=pltpu.VMEM)] * count


def call(body, out_shape, inputs, limit, scalars=(), scratch=(), flops=0):
    many = isinstance(out_shape, (tuple, list))
    return pl.pallas_call(
        body,
        out_shape=out_shape,
        in_specs=[pl.BlockSpec(memory_space=pltpu.SMEM)] * len(scalars) + vmem(len(inputs)),
        out_specs=tuple(vmem(len(out_shape))) if many else vmem(1)[0],
        scratch_shapes=list(scratch),
        compiler_params=pltpu.CompilerParams(vmem_limit_bytes=limit),
        cost_estimate=pl.CostEstimate(flops=flops, transcendentals=0, bytes_accessed=0) if flops else None,
    )(*scalars, *inputs)


def request_kernel(rows_held, hash_ref, out_ref):
    row = hash_ref[...]
    owner = row // rows_held
    local = row - owner * rows_held
    owner_rows = jnp.broadcast_to(owner.astype(f32), (LANES, LANES))
    owner_cols = owner_rows.T
    earlier = (owner_rows == owner_cols) & (iota((LANES, LANES), 0) < iota((LANES, LANES), 1))
    slot = jnp.sum(earlier.astype(f32), axis=0, keepdims=True)
    position = owner * 2 + slot.astype(jnp.int32)
    place = iota((LANES, LANES), 0)
    local_f = local.astype(f32)
    zero = jnp.zeros((LANES, LANES), f32)
    ask0 = jnp.sum(jnp.where(position == 2 * place, local_f, zero), axis=1, keepdims=True)
    ask1 = jnp.sum(jnp.where(position == 2 * place + 1, local_f, zero), axis=1, keepdims=True)
    asks = jnp.where(iota((LANES, LANES), 1) < LANES // 2, ask0, ask1)
    where = jnp.broadcast_to(position.astype(f32), (LANES, LANES))
    both = jnp.stack([where, asks], axis=1)
    out_ref[...] = both.reshape(2 * LANES, LANES).astype(bf16)


def gather_kernel(asked_ref, table_ref, out_ref):
    asked = asked_ref[...].astype(f32)
    rows = asked.shape[0]
    even = (iota((rows, 1), 0) % 2) == 0
    ahead = pltpu.roll(asked, rows - 1, 0)
    index = jnp.where(even, ahead[:, 0:1], asked[:, LANES - 1 :])
    held = table_ref.shape[0]
    chosen = (index.astype(jnp.int32) == iota((rows, held), 1)).astype(f32).astype(bf16)
    found = jnp.dot(chosen, table_ref[...], preferred_element_type=f32)
    turns = [found[chip // 2 * 8 : chip // 2 * 8 + 8] for chip in chip_order()]
    out_ref[...] = jnp.concatenate(turns, axis=0).astype(bf16)


def place_kernel(heads, where_ref, asked_ref, arrived_ref, out_ref):
    core = where_ref[0] & 1
    start = pl.multiple_of((where_ref[0] >> 2) * 8, 8)
    position = asked_ref[pl.ds(start, 8), :].astype(jnp.int32)
    target = turn_of(position >> 2) * 8 + (position & 1)
    target = jnp.where(((position >> 1) & 1) == core, target, -8).astype(f32)
    arrived = arrived_ref[...]
    slots = arrived.shape[0]
    width = arrived.shape[1]
    for k, head in enumerate(heads):
        column = jnp.broadcast_to(target[2 * head : 2 * head + 1, :], (LANES, LANES)).T
        column = column[:, 0:1].astype(jnp.int32) + 2 * head
        chosen = (column == iota((LANES, slots), 1)).astype(f32).astype(bf16)
        found = jnp.dot(chosen, arrived, preferred_element_type=f32)
        out_ref[:, k * width : (k + 1) * width] = found.astype(bf16)


def row_of_sums(terms):
    parts = terms[:, 0:LANES]
    for k in range(1, terms.shape[1] // LANES):
        parts = parts + terms[:, k * LANES : (k + 1) * LANES]
    return jnp.sum(parts.T, axis=0, keepdims=True)


def first_kernel(mine_ref, other_ref, weight_ref, out_ref):
    memory = mine_ref[...] + other_ref[...]
    out_ref[...] = jnp.dot(memory, weight_ref[: memory.shape[1], :], preferred_element_type=f32)


def second_kernel(mine_ref, other_ref, weight_ref, first_ref, out_ref):
    memory = mine_ref[...] + other_ref[...]
    more = jnp.dot(memory, weight_ref[memory.shape[1] :, :], preferred_element_type=f32)
    out_ref[...] = first_ref[...] + more


def key_kernel(mine_ref, other_ref, weight_ref, first_ref, hidden_ref, hgain_ref, kgain_ref, sums_ref):
    memory = mine_ref[...] + other_ref[...]
    key = first_ref[...] + jnp.dot(memory, weight_ref[memory.shape[1] :, :], preferred_element_type=f32)
    hidden = hidden_ref[...].astype(f32)
    sums = [
        row_of_sums(hidden * hidden),
        row_of_sums(key * key),
        row_of_sums((hidden * hgain_ref[...]) * (key * kgain_ref[...])),
    ]
    sums_ref[...] = jnp.concatenate(sums + [jnp.zeros((5, LANES), f32)], axis=0)


def join_kernel(chunks, here_ref, there_ref, hidden_ref, projected_ref, out_ref, joined_ref, sems):
    sums = here_ref[...] + there_ref[...]
    hidden_power = sums[0:1] / D
    key_power = sums[1:2] / D
    agreement = sums[2:3] * lax.rsqrt(hidden_power + EPSILON) * lax.rsqrt(key_power + EPSILON)
    gate = jax.nn.sigmoid(agreement / math.sqrt(D))
    gate = jnp.broadcast_to(gate, (LANES, LANES)).T[:, 0:1]
    rows = LANES // chunks
    copies = []
    for k in range(chunks):
        part = slice(k * rows, (k + 1) * rows)
        joined = hidden_ref[part, :].astype(f32) + gate[part] * projected_ref[part, :]
        joined_ref[part, :] = joined.astype(bf16)
        copy = pltpu.make_async_copy(joined_ref.at[part, :], out_ref.at[part, :], sems.at[k])
        copy.start()
        copies.append(copy)
    for copy in copies:
        copy.wait()


def local(hidden, hash_rows, memory_table, key_weight, value_weight, hidden_gain, key_gain):
    groups = lax.axis_size("dp")
    tensor = lax.axis_size("tensor")
    devices = groups * tensor
    rows_held, row_width = memory_table.shape
    shape = jax.ShapeDtypeStruct

    here = lax.axis_index(BOTH).astype(jnp.int32).reshape(1)
    hash_rows, here, hidden_gain, key_gain = lax.optimization_barrier((hash_rows, here, hidden_gain, key_gain))
    message = call(
        lambda *refs: request_kernel(rows_held, *refs),
        shape((2 * devices, LANES), bf16),
        [hash_rows.reshape(1, LANES)],
        4 * MIB,
        flops=COVER,
    )
    asked = lax.all_to_all(message.reshape(devices, 2, LANES), BOTH, 0, 0, tiled=True)
    asked = asked.reshape(2 * devices, LANES)
    sent = call(gather_kernel, shape((4 * devices, row_width), bf16), [asked, memory_table], 6 * MIB, flops=COVER)
    same_core = [[2 * chip + core for chip in chip_order()] for core in range(2)]
    arrived = lax.all_to_all(
        sent.reshape(devices // 2, 8, row_width), BOTH, 0, 0, axis_index_groups=same_core, tiled=True
    ).reshape(4 * devices, row_width)
    halves = []
    for heads in ((0, 1), (2, 3)):
        mine = call(
            lambda *refs, heads=heads: place_kernel(heads, *refs),
            shape((LANES, 2 * row_width), bf16),
            [asked, arrived],
            6 * MIB,
            scalars=[here],
        )
        halves.append((mine, lax.ppermute(mine, "tensor", [(k, k ^ 1) for k in range(tensor)])))
    columns = key_weight.shape[1]
    work = 2 * LANES * 2 * row_width * columns
    key_weight = pltpu.with_memory_space_constraint(key_weight, pltpu.VMEM)
    value_weight = pltpu.with_memory_space_constraint(value_weight, pltpu.VMEM)
    partial = shape((LANES, columns), f32)
    key = call(
        lambda mine, other, weight, _, out: first_kernel(mine, other, weight, out),
        partial,
        [*halves[0], key_weight, value_weight],
        6 * MIB,
        flops=work,
    )
    sums = call(
        key_kernel,
        shape((8, LANES), f32),
        [*halves[1], key_weight, key, hidden, hidden_gain.reshape(1, columns), key_gain.reshape(1, columns)],
        6 * MIB,
        flops=work,
    )
    sums_there = lax.ppermute(sums, "tensor", [(k, k ^ 1) for k in range(tensor)])
    value = call(first_kernel, partial, [*halves[0], value_weight], 6 * MIB, flops=work)
    value, sums_there = lax.optimization_barrier((value, sums_there))
    sums = sums + sums_there
    sums_there = lax.ppermute(sums, "tensor", [(k, k ^ 2) for k in range(tensor)])
    value, sums = lax.optimization_barrier((value, sums))
    projected = call(second_kernel, partial, [*halves[1], value_weight, value], 6 * MIB, flops=work)
    chunks = 4
    return pl.pallas_call(
        lambda *refs: join_kernel(chunks, *refs),
        out_shape=shape(hidden.shape, bf16),
        in_specs=vmem(4),
        out_specs=pl.BlockSpec(memory_space=pl.ANY),
        scratch_shapes=[pltpu.VMEM(hidden.shape, bf16), pltpu.SemaphoreType.DMA((chunks,))],
        compiler_params=pltpu.CompilerParams(vmem_limit_bytes=6 * MIB),
    )(sums, sums_there, hidden, projected)


def solution(mesh):
    return jax.shard_map(
        local,
        mesh=mesh,
        in_specs=(
            P("dp", "tensor"),
            P("dp", "tensor"),
            P(("dp", "tensor"), None),
            P(None, "tensor"),
            P(None, "tensor"),
            P("tensor"),
            P("tensor"),
        ),
        out_specs=P("dp", "tensor"),
        check_vma=False,
    )
```

```python
import math

import jax
import jax.numpy as jnp
from jax import lax
from jax.experimental import pallas as pl
from jax.experimental.pallas import tpu as pltpu
from jax.sharding import PartitionSpec as P

D = 7168
LANES = 128
EPSILON = 1e-06
COVER = 20_000_000_000
BOTH = ("dp", "tensor")
MIB = 1024 * 1024

f32 = jnp.float32
bf16 = jnp.bfloat16


def chip_order():
    order = []
    for k in range(64):
        a, b, c = k % 4, (k // 4) % 4, k // 16
        order.append(a * 16 + (a + b) % 4 * 4 + (a + b + c) % 4)
    return order


def turn_of(chip):
    z, y, x = chip >> 4, (chip >> 2) & 3, chip & 3
    return z + ((y - z) & 3) * 4 + ((x - y) & 3) * 16


def iota(shape, dim):
    return lax.broadcasted_iota(jnp.int32, shape, dim)


def vmem(count):
    return [pl.BlockSpec(memory_space=pltpu.VMEM)] * count


def call(body, out_shape, inputs, limit, scalars=(), scratch=(), flops=0):
    many = isinstance(out_shape, (tuple, list))
    return pl.pallas_call(
        body,
        out_shape=out_shape,
        in_specs=[pl.BlockSpec(memory_space=pltpu.SMEM)] * len(scalars) + vmem(len(inputs)),
        out_specs=tuple(vmem(len(out_shape))) if many else vmem(1)[0],
        scratch_shapes=list(scratch),
        compiler_params=pltpu.CompilerParams(vmem_limit_bytes=limit),
        cost_estimate=pl.CostEstimate(flops=flops, transcendentals=0, bytes_accessed=0) if flops else None,
    )(*scalars, *inputs)


def request_kernel(rows_held, hash_ref, out_ref):
    row = hash_ref[...]
    owner = row // rows_held
    local = row - owner * rows_held
    owner_rows = jnp.broadcast_to(owner.astype(f32), (LANES, LANES))
    owner_cols = owner_rows.T
    earlier = (owner_rows == owner_cols) & (iota((LANES, LANES), 0) < iota((LANES, LANES), 1))
    slot = jnp.sum(earlier.astype(f32), axis=0, keepdims=True)
    position = owner * 2 + slot.astype(jnp.int32)
    place = iota((LANES, LANES), 0)
    local_f = local.astype(f32)
    zero = jnp.zeros((LANES, LANES), f32)
    ask0 = jnp.sum(jnp.where(position == 2 * place, local_f, zero), axis=1, keepdims=True)
    ask1 = jnp.sum(jnp.where(position == 2 * place + 1, local_f, zero), axis=1, keepdims=True)
    asks = jnp.where(iota((LANES, LANES), 1) < LANES // 2, ask0, ask1)
    where = jnp.broadcast_to(position.astype(f32), (LANES, LANES))
    both = jnp.stack([where, asks], axis=1)
    out_ref[...] = both.reshape(2 * LANES, LANES).astype(bf16)


def gather_kernel(asked_ref, table_ref, out_ref):
    asked = asked_ref[...].astype(f32)
    rows = asked.shape[0]
    even = (iota((rows, 1), 0) % 2) == 0
    ahead = pltpu.roll(asked, rows - 1, 0)
    index = jnp.where(even, ahead[:, 0:1], asked[:, LANES - 1 :])
    held = table_ref.shape[0]
    chosen = (index.astype(jnp.int32) == iota((rows, held), 1)).astype(f32).astype(bf16)
    found = jnp.dot(chosen, table_ref[...], preferred_element_type=f32)
    turns = [found[chip // 2 * 8 : chip // 2 * 8 + 8] for chip in chip_order()]
    out_ref[...] = jnp.concatenate(turns, axis=0).astype(bf16)


def place_kernel(heads, where_ref, asked_ref, arrived_ref, out_ref):
    core = where_ref[0] & 1
    start = pl.multiple_of((where_ref[0] >> 2) * 8, 8)
    position = asked_ref[pl.ds(start, 8), :].astype(jnp.int32)
    target = turn_of(position >> 2) * 8 + (position & 1)
    target = jnp.where(((position >> 1) & 1) == core, target, -8).astype(f32)
    arrived = arrived_ref[...]
    slots = arrived.shape[0]
    width = arrived.shape[1]
    chosen = []
    for head in heads:
        column = jnp.broadcast_to(target[2 * head : 2 * head + 1, :], (LANES, LANES)).T
        column = column[:, 0:1].astype(jnp.int32) + 2 * head
        chosen.append((column == iota((LANES, slots), 1)).astype(f32).astype(bf16))
    found = jnp.dot(jnp.concatenate(chosen, axis=0), arrived, preferred_element_type=f32).astype(bf16)
    for k in range(len(heads)):
        out_ref[:, k * width : (k + 1) * width] = found[k * LANES : (k + 1) * LANES]


def row_of_sums(terms):
    parts = terms[:, 0:LANES]
    for k in range(1, terms.shape[1] // LANES):
        parts = parts + terms[:, k * LANES : (k + 1) * LANES]
    return jnp.sum(parts.T, axis=0, keepdims=True)


def first_kernel(mine_ref, other_ref, weight_ref, out_ref):
    memory = mine_ref[...] + other_ref[...]
    out_ref[...] = jnp.dot(memory, weight_ref[: memory.shape[1], :], preferred_element_type=f32)


def value_kernel(mine0_ref, other0_ref, mine1_ref, other1_ref, weight_ref, out_ref):
    memory = jnp.concatenate([mine0_ref[...] + other0_ref[...], mine1_ref[...] + other1_ref[...]], axis=1)
    out_ref[...] = jnp.dot(memory, weight_ref[...], preferred_element_type=f32)


def key_kernel(mine_ref, other_ref, weight_ref, first_ref, hidden_ref, hgain_ref, kgain_ref, sums_ref):
    memory = mine_ref[...] + other_ref[...]
    key = first_ref[...] + jnp.dot(memory, weight_ref[memory.shape[1] :, :], preferred_element_type=f32)
    hidden = hidden_ref[...].astype(f32)
    sums = [
        row_of_sums(hidden * hidden),
        row_of_sums(key * key),
        row_of_sums((hidden * hgain_ref[...]) * (key * kgain_ref[...])),
    ]
    sums_ref[...] = jnp.concatenate(sums + [jnp.zeros((5, LANES), f32)], axis=0)


def join_kernel(chunks, s0_ref, s1_ref, s2_ref, s3_ref, hidden_ref, projected_ref, out_ref, joined_ref, sems):
    sums = (s0_ref[...] + s1_ref[...]) + (s2_ref[...] + s3_ref[...])
    hidden_power = sums[0:1] / D
    key_power = sums[1:2] / D
    agreement = sums[2:3] * lax.rsqrt(hidden_power + EPSILON) * lax.rsqrt(key_power + EPSILON)
    gate = jax.nn.sigmoid(agreement / math.sqrt(D))
    gate = jnp.broadcast_to(gate, (LANES, LANES)).T[:, 0:1]
    rows = LANES // chunks
    copies = []
    for k in range(chunks):
        part = slice(k * rows, (k + 1) * rows)
        joined = hidden_ref[part, :].astype(f32) + gate[part] * projected_ref[part, :]
        joined_ref[part, :] = joined.astype(bf16)
        copy = pltpu.make_async_copy(joined_ref.at[part, :], out_ref.at[part, :], sems.at[k])
        copy.start()
        copies.append(copy)
    for copy in copies:
        copy.wait()


def local(hidden, hash_rows, memory_table, key_weight, value_weight, hidden_gain, key_gain):
    groups = lax.axis_size("dp")
    tensor = lax.axis_size("tensor")
    devices = groups * tensor
    rows_held, row_width = memory_table.shape
    shape = jax.ShapeDtypeStruct

    here = lax.axis_index(BOTH).astype(jnp.int32).reshape(1)
    hash_rows, here, hidden_gain, key_gain = lax.optimization_barrier((hash_rows, here, hidden_gain, key_gain))
    message = call(
        lambda *refs: request_kernel(rows_held, *refs),
        shape((2 * devices, LANES), bf16),
        [hash_rows.reshape(1, LANES)],
        4 * MIB,
        flops=COVER,
    )
    asked = lax.all_to_all(message.reshape(devices, 2, LANES), BOTH, 0, 0, tiled=True)
    asked = asked.reshape(2 * devices, LANES)
    sent = call(gather_kernel, shape((4 * devices, row_width), bf16), [asked, memory_table], 6 * MIB, flops=COVER)
    same_core = [[2 * chip + core for chip in chip_order()] for core in range(2)]
    arrived = lax.all_to_all(
        sent.reshape(devices // 2, 8, row_width), BOTH, 0, 0, axis_index_groups=same_core, tiled=True
    ).reshape(4 * devices, row_width)
    halves = []
    for heads in ((0, 1), (2, 3)):
        mine = call(
            lambda *refs, heads=heads: place_kernel(heads, *refs),
            shape((LANES, 2 * row_width), bf16),
            [asked, arrived],
            6 * MIB,
            scalars=[here],
        )
        halves.append((mine, lax.ppermute(mine, "tensor", [(k, k ^ 1) for k in range(tensor)])))
    columns = key_weight.shape[1]
    work = 2 * LANES * 2 * row_width * columns
    key_weight = pltpu.with_memory_space_constraint(key_weight, pltpu.VMEM)
    value_weight = pltpu.with_memory_space_constraint(value_weight, pltpu.VMEM)
    partial = shape((LANES, columns), f32)
    key = call(
        lambda mine, other, weight, _, out: first_kernel(mine, other, weight, out),
        partial,
        [*halves[0], key_weight, value_weight],
        6 * MIB,
        flops=work,
    )
    sums = call(
        key_kernel,
        shape((8, LANES), f32),
        [*halves[1], key_weight, key, hidden, hidden_gain.reshape(1, columns), key_gain.reshape(1, columns)],
        6 * MIB,
        flops=work,
    )
    others = [lax.ppermute(sums, "tensor", [(k, k ^ d) for k in range(tensor)]) for d in (3, 2, 1)]
    projected = call(value_kernel, partial, [*halves[0], *halves[1], value_weight], 6 * MIB, flops=2 * work)
    chunks = 4
    return pl.pallas_call(
        lambda *refs: join_kernel(chunks, *refs),
        out_shape=shape(hidden.shape, bf16),
        in_specs=vmem(6),
        out_specs=pl.BlockSpec(memory_space=pl.ANY),
        scratch_shapes=[pltpu.VMEM(hidden.shape, bf16), pltpu.SemaphoreType.DMA((chunks,))],
        compiler_params=pltpu.CompilerParams(vmem_limit_bytes=6 * MIB),
    )(sums, *others, hidden, projected)


def solution(mesh):
    return jax.shard_map(
        local,
        mesh=mesh,
        in_specs=(
            P("dp", "tensor"),
            P("dp", "tensor"),
            P(("dp", "tensor"), None),
            P(None, "tensor"),
            P(None, "tensor"),
            P("tensor"),
            P("tensor"),
        ),
        out_specs=P("dp", "tensor"),
        check_vma=False,
    )
```

```python
import math

import jax
import jax.numpy as jnp
from jax import lax
from jax.experimental import pallas as pl
from jax.experimental.pallas import tpu as pltpu
from jax.sharding import PartitionSpec as P

D = 7168
LANES = 128
EPSILON = 1e-06
COVER = 20_000_000_000
BOTH = ("dp", "tensor")
MIB = 1024 * 1024

f32 = jnp.float32
bf16 = jnp.bfloat16


def chip_order():
    order = []
    for k in range(64):
        a, b, c = k % 4, (k // 4) % 4, k // 16
        order.append(a * 16 + (a + b) % 4 * 4 + (a + b + c) % 4)
    return order


def turn_of(chip):
    z, y, x = chip >> 4, (chip >> 2) & 3, chip & 3
    return z + ((y - z) & 3) * 4 + ((x - y) & 3) * 16


def iota(shape, dim):
    return lax.broadcasted_iota(jnp.int32, shape, dim)


def vmem(count):
    return [pl.BlockSpec(memory_space=pltpu.VMEM)] * count


def call(body, out_shape, inputs, limit, scalars=(), scratch=(), flops=0):
    many = isinstance(out_shape, (tuple, list))
    return pl.pallas_call(
        body,
        out_shape=out_shape,
        in_specs=[pl.BlockSpec(memory_space=pltpu.SMEM)] * len(scalars) + vmem(len(inputs)),
        out_specs=tuple(vmem(len(out_shape))) if many else vmem(1)[0],
        scratch_shapes=list(scratch),
        compiler_params=pltpu.CompilerParams(vmem_limit_bytes=limit),
        cost_estimate=pl.CostEstimate(flops=flops, transcendentals=0, bytes_accessed=0) if flops else None,
    )(*scalars, *inputs)


def request_kernel(rows_held, hash_ref, out_ref):
    row = hash_ref[...]
    owner = row // rows_held
    local = (row - owner * rows_held).astype(f32)
    owner_rows = jnp.broadcast_to(owner.astype(f32), (LANES, LANES))
    owner_cols = owner_rows.T
    earlier = (owner_rows == owner_cols) & (iota((LANES, LANES), 0) < iota((LANES, LANES), 1))
    slot = jnp.sum(earlier.astype(f32), axis=0, keepdims=True)
    position = owner * 2 + slot.astype(jnp.int32)
    rows = out_ref.shape[0]
    asks = jnp.where(position == iota((rows, LANES), 0), local, jnp.zeros((rows, LANES), f32))
    asks = jnp.sum(asks, axis=1, keepdims=True)
    where = position.astype(f32)
    turned = pltpu.roll(where, LANES // 2, 1)
    first = (iota((rows, LANES), 0) & 3) == 0
    message = jnp.where(iota((rows, LANES), 1) < LANES // 2, asks, jnp.where(first, turned, where))
    out_ref[...] = message.astype(bf16)


def gather_kernel(here_ref, asked_ref, mine_ref, other_ref, out_ref):
    core = here_ref[0] & 1
    index = asked_ref[...].astype(jnp.int32)[:, 0:1]
    rows = index.shape[0]
    held = mine_ref.shape[0]
    is_mine = ((iota((rows, 1), 0) >> 1) & 1) == core
    lanes = iota((rows, held), 1)
    from_mine = (jnp.where(is_mine, index, -1) == lanes).astype(f32).astype(bf16)
    from_other = (jnp.where(is_mine, -1, index) == lanes).astype(f32).astype(bf16)
    found = jnp.dot(from_mine, mine_ref[...], preferred_element_type=f32)
    found = found + jnp.dot(from_other, other_ref[...], preferred_element_type=f32)
    turns = [found[chip // 2 * 8 : chip // 2 * 8 + 8] for chip in chip_order()]
    out_ref[...] = jnp.concatenate(turns, axis=0).astype(bf16)


def place_kernel(here_ref, asked_ref, arrived_ref, out_ref):
    start = pl.multiple_of((here_ref[0] >> 2) * 8, 8)
    asked = asked_ref[pl.ds(start, 8), :].astype(f32)
    arrived = arrived_ref[...]
    slots = arrived.shape[0]
    width = arrived.shape[1]
    low = iota((1, LANES), 1) < LANES // 2
    turned = pltpu.roll(asked, LANES // 2, 1)
    for x in range(2):
        position = jnp.where(low, turned[4 * x : 4 * x + 1], asked[4 * x + 1 : 4 * x + 2]).astype(jnp.int32)
        target = turn_of(position >> 2) * 8 + x * 4 + (position & 3)
        column = jnp.broadcast_to(target.astype(f32), (LANES, LANES)).T[:, 0:1].astype(jnp.int32)
        chosen = (column == iota((LANES, slots), 1)).astype(f32).astype(bf16)
        found = jnp.dot(chosen, arrived, preferred_element_type=f32)
        out_ref[:, x * width : (x + 1) * width] = found.astype(bf16)


def row_of_sums(terms):
    parts = terms[:, 0:LANES]
    for k in range(1, terms.shape[1] // LANES):
        parts = parts + terms[:, k * LANES : (k + 1) * LANES]
    return jnp.sum(parts.T, axis=0, keepdims=True)


def rows_of_heads(weight_ref, core):
    width = weight_ref.shape[0] // 4
    starts = [pl.multiple_of((2 * x + core) * width, LANES) for x in range(2)]
    return jnp.concatenate([weight_ref[pl.ds(start, width), :] for start in starts], axis=0)


def own_key_kernel(here_ref, mine_ref, weight_ref, _, out_ref):
    out_ref[...] = jnp.dot(
        mine_ref[...], rows_of_heads(weight_ref, here_ref[0] & 1), preferred_element_type=f32
    )


def key_kernel(here_ref, other_ref, weight_ref, own_ref, hidden_ref, hgain_ref, kgain_ref, sums_ref):
    weight = rows_of_heads(weight_ref, 1 - (here_ref[0] & 1))
    key = own_ref[...] + jnp.dot(other_ref[...], weight, preferred_element_type=f32)
    hidden = hidden_ref[...].astype(f32)
    sums = [
        row_of_sums(hidden * hidden),
        row_of_sums(key * key),
        row_of_sums((hidden * hgain_ref[...]) * (key * kgain_ref[...])),
    ]
    sums_ref[...] = jnp.concatenate(sums + [jnp.zeros((5, LANES), f32)], axis=0)


def value_kernel(here_ref, mine_ref, other_ref, weight_ref, out_ref):
    core = here_ref[0] & 1
    projected = jnp.dot(mine_ref[...], rows_of_heads(weight_ref, core), preferred_element_type=f32)
    more = jnp.dot(other_ref[...], rows_of_heads(weight_ref, 1 - core), preferred_element_type=f32)
    out_ref[...] = projected + more


def join_kernel(chunks, s0_ref, s1_ref, s2_ref, s3_ref, hidden_ref, projected_ref, out_ref, joined_ref, sems):
    sums = (s0_ref[...] + s1_ref[...]) + (s2_ref[...] + s3_ref[...])
    hidden_power = sums[0:1] / D
    key_power = sums[1:2] / D
    agreement = sums[2:3] * lax.rsqrt(hidden_power + EPSILON) * lax.rsqrt(key_power + EPSILON)
    gate = jax.nn.sigmoid(agreement / math.sqrt(D))
    gate = jnp.broadcast_to(gate, (LANES, LANES)).T[:, 0:1]
    rows = LANES // chunks
    copies = []
    for k in range(chunks):
        part = slice(k * rows, (k + 1) * rows)
        joined = hidden_ref[part, :].astype(f32) + gate[part] * projected_ref[part, :]
        joined_ref[part, :] = joined.astype(bf16)
        copy = pltpu.make_async_copy(joined_ref.at[part, :], out_ref.at[part, :], sems.at[k])
        copy.start()
        copies.append(copy)
    for copy in copies:
        copy.wait()


def local(hidden, hash_rows, memory_table, key_weight, value_weight, hidden_gain, key_gain):
    groups = lax.axis_size("dp")
    tensor = lax.axis_size("tensor")
    devices = groups * tensor
    rows_held, row_width = memory_table.shape
    shape = jax.ShapeDtypeStruct

    here = lax.axis_index(BOTH).astype(jnp.int32).reshape(1)
    hash_rows, here, hidden_gain, key_gain = lax.optimization_barrier((hash_rows, here, hidden_gain, key_gain))
    table_there = lax.ppermute(memory_table, "tensor", [(k, k ^ 1) for k in range(tensor)])
    chips = devices // 2
    message = call(
        lambda *refs: request_kernel(rows_held, *refs),
        shape((4 * chips, LANES), bf16),
        [hash_rows.reshape(1, LANES)],
        4 * MIB,
        flops=COVER,
    )
    in_turn = [[2 * chip + core for chip in chip_order()] for core in range(2)]
    in_place = [[2 * chip + core for chip in range(chips)] for core in range(2)]
    asked = lax.all_to_all(
        message.reshape(chips, 4, LANES), BOTH, 0, 0, axis_index_groups=in_place, tiled=True
    ).reshape(4 * chips, LANES)
    sent = call(
        gather_kernel,
        shape((8 * chips, row_width), bf16),
        [asked, memory_table, table_there],
        6 * MIB,
        scalars=[here],
        flops=COVER,
    )
    arrived = lax.all_to_all(
        sent.reshape(chips, 8, row_width), BOTH, 0, 0, axis_index_groups=in_turn, tiled=True
    ).reshape(8 * chips, row_width)
    mine = call(place_kernel, shape((LANES, 2 * row_width), bf16), [asked, arrived], 6 * MIB, scalars=[here])
    other = lax.ppermute(mine, "tensor", [(k, k ^ 1) for k in range(tensor)])
    columns = key_weight.shape[1]
    work = 2 * LANES * 2 * row_width * columns
    key_weight = pltpu.with_memory_space_constraint(key_weight, pltpu.VMEM)
    value_weight = pltpu.with_memory_space_constraint(value_weight, pltpu.VMEM)
    partial = shape((LANES, columns), f32)
    key = call(
        own_key_kernel, partial, [mine, key_weight, value_weight], 6 * MIB, scalars=[here], flops=work
    )
    sums = call(
        key_kernel,
        shape((8, LANES), f32),
        [other, key_weight, key, hidden, hidden_gain.reshape(1, columns), key_gain.reshape(1, columns)],
        6 * MIB,
        scalars=[here],
        flops=work,
    )
    others = [lax.ppermute(sums, "tensor", [(k, k ^ d) for k in range(tensor)]) for d in (3, 2, 1)]
    projected = call(value_kernel, partial, [mine, other, value_weight], 6 * MIB, scalars=[here], flops=2 * work)
    chunks = 4
    return pl.pallas_call(
        lambda *refs: join_kernel(chunks, *refs),
        out_shape=shape(hidden.shape, bf16),
        in_specs=vmem(6),
        out_specs=pl.BlockSpec(memory_space=pl.ANY),
        scratch_shapes=[pltpu.VMEM(hidden.shape, bf16), pltpu.SemaphoreType.DMA((chunks,))],
        compiler_params=pltpu.CompilerParams(vmem_limit_bytes=6 * MIB),
    )(sums, *others, hidden, projected)


def solution(mesh):
    return jax.shard_map(
        local,
        mesh=mesh,
        in_specs=(
            P("dp", "tensor"),
            P("dp", "tensor"),
            P(("dp", "tensor"), None),
            P(None, "tensor"),
            P(None, "tensor"),
            P("tensor"),
            P("tensor"),
        ),
        out_specs=P("dp", "tensor"),
        check_vma=False,
    )
```

```python
import math

import jax
import jax.numpy as jnp
from jax import lax
from jax.experimental import pallas as pl
from jax.experimental.pallas import tpu as pltpu
from jax.sharding import PartitionSpec as P

D = 7168
LANES = 128
EPSILON = 1e-06
COVER = 20_000_000_000
BOTH = ("dp", "tensor")
MIB = 1024 * 1024

f32 = jnp.float32
bf16 = jnp.bfloat16


def chip_order():
    order = []
    for k in range(64):
        a, b, c = k % 4, (k // 4) % 4, k // 16
        order.append(a * 16 + (a + b) % 4 * 4 + (a + b + c) % 4)
    return order


def turn_of(chip):
    z, y, x = chip >> 4, (chip >> 2) & 3, chip & 3
    return z + ((y - z) & 3) * 4 + ((x - y) & 3) * 16


def iota(shape, dim):
    return lax.broadcasted_iota(jnp.int32, shape, dim)


def vmem(count):
    return [pl.BlockSpec(memory_space=pltpu.VMEM)] * count


def call(body, out_shape, inputs, limit, scalars=(), scratch=(), flops=0):
    many = isinstance(out_shape, (tuple, list))
    return pl.pallas_call(
        body,
        out_shape=out_shape,
        in_specs=[pl.BlockSpec(memory_space=pltpu.SMEM)] * len(scalars) + vmem(len(inputs)),
        out_specs=tuple(vmem(len(out_shape))) if many else vmem(1)[0],
        scratch_shapes=list(scratch),
        compiler_params=pltpu.CompilerParams(vmem_limit_bytes=limit),
        cost_estimate=pl.CostEstimate(flops=flops, transcendentals=0, bytes_accessed=0) if flops else None,
    )(*scalars, *inputs)


def request_kernel(rows_held, hash_ref, out_ref):
    row = hash_ref[...]
    owner = row // rows_held
    local = (row - owner * rows_held).astype(f32)
    owner_rows = jnp.broadcast_to(owner.astype(f32), (LANES, LANES))
    owner_cols = owner_rows.T
    earlier = (owner_rows == owner_cols) & (iota((LANES, LANES), 0) < iota((LANES, LANES), 1))
    slot = jnp.sum(earlier.astype(f32), axis=0, keepdims=True)
    position = owner * 2 + slot.astype(jnp.int32)
    rows = out_ref.shape[0]
    asks = jnp.where(position == iota((rows, LANES), 0), local, jnp.zeros((rows, LANES), f32))
    asks = jnp.sum(asks, axis=1, keepdims=True)
    where = position.astype(f32)
    turned = pltpu.roll(where, LANES // 2, 1)
    first = (iota((rows, LANES), 0) & 3) == 0
    message = jnp.where(iota((rows, LANES), 1) < LANES // 2, asks, jnp.where(first, turned, where))
    out_ref[...] = message.astype(bf16)


def gather_kernel(here_ref, asked_ref, mine_ref, other_ref, out_ref):
    core = here_ref[0] & 1
    index = asked_ref[...].astype(jnp.int32)[:, 0:1]
    rows = index.shape[0]
    held = mine_ref.shape[0]
    is_mine = ((iota((rows, 1), 0) >> 1) & 1) == core
    swapped = jnp.where(is_mine, index, index + held)
    chosen = (swapped == iota((rows, 2 * held), 1)).astype(f32).astype(bf16)
    table = jnp.concatenate([mine_ref[...], other_ref[...]], axis=0)
    found = jnp.dot(chosen, table, preferred_element_type=f32)
    turns = [found[chip // 2 * 8 : chip // 2 * 8 + 8] for chip in chip_order()]
    out_ref[...] = jnp.concatenate(turns, axis=0).astype(bf16)


def place_kernel(here_ref, asked_ref, arrived_ref, out_ref):
    start = pl.multiple_of((here_ref[0] >> 2) * 8, 8)
    asked = asked_ref[pl.ds(start, 8), :].astype(f32)
    arrived = arrived_ref[...]
    slots = arrived.shape[0]
    width = arrived.shape[1]
    low = iota((1, LANES), 1) < LANES // 2
    turned = pltpu.roll(asked, LANES // 2, 1)
    for x in range(2):
        position = jnp.where(low, turned[4 * x : 4 * x + 1], asked[4 * x + 1 : 4 * x + 2]).astype(jnp.int32)
        target = turn_of(position >> 2) * 8 + x * 4 + (position & 3)
        chosen = (target == iota((slots, LANES), 0)).astype(f32).astype(bf16)
        found = lax.dot_general(chosen, arrived, (((0,), (0,)), ((), ())), preferred_element_type=f32)
        out_ref[:, x * width : (x + 1) * width] = found.astype(bf16)


def row_of_sums(terms):
    parts = terms[:, 0:LANES]
    for k in range(1, terms.shape[1] // LANES):
        parts = parts + terms[:, k * LANES : (k + 1) * LANES]
    return jnp.sum(parts.T, axis=0, keepdims=True)


def rows_of_heads(weight_ref, core):
    width = weight_ref.shape[0] // 4
    starts = [pl.multiple_of((2 * x + core) * width, LANES) for x in range(2)]
    return jnp.concatenate([weight_ref[pl.ds(start, width), :] for start in starts], axis=0)


def own_key_kernel(here_ref, mine_ref, weight_ref, _, out_ref):
    out_ref[...] = jnp.dot(
        mine_ref[...], rows_of_heads(weight_ref, here_ref[0] & 1), preferred_element_type=f32
    )


def key_kernel(here_ref, other_ref, weight_ref, own_ref, hidden_ref, hgain_ref, kgain_ref, sums_ref):
    weight = rows_of_heads(weight_ref, 1 - (here_ref[0] & 1))
    key = own_ref[...] + jnp.dot(other_ref[...], weight, preferred_element_type=f32)
    hidden = hidden_ref[...].astype(f32)
    sums = [
        row_of_sums(hidden * hidden),
        row_of_sums(key * key),
        row_of_sums((hidden * hgain_ref[...]) * (key * kgain_ref[...])),
    ]
    sums_ref[...] = jnp.concatenate(sums + [jnp.zeros((5, LANES), f32)], axis=0)


def value_kernel(here_ref, mine_ref, other_ref, weight_ref, out_ref):
    core = here_ref[0] & 1
    projected = jnp.dot(mine_ref[...], rows_of_heads(weight_ref, core), preferred_element_type=f32)
    more = jnp.dot(other_ref[...], rows_of_heads(weight_ref, 1 - core), preferred_element_type=f32)
    out_ref[...] = projected + more


def join_kernel(chunks, s0_ref, s1_ref, s2_ref, s3_ref, hidden_ref, projected_ref, out_ref, joined_ref, sems):
    sums = (s0_ref[...] + s1_ref[...]) + (s2_ref[...] + s3_ref[...])
    hidden_power = sums[0:1] / D
    key_power = sums[1:2] / D
    agreement = sums[2:3] * lax.rsqrt(hidden_power + EPSILON) * lax.rsqrt(key_power + EPSILON)
    gate = jax.nn.sigmoid(agreement / math.sqrt(D))
    gate = jnp.broadcast_to(gate, (LANES, LANES)).T[:, 0:1]
    rows = LANES // chunks
    copies = []
    for k in range(chunks):
        part = slice(k * rows, (k + 1) * rows)
        joined = hidden_ref[part, :].astype(f32) + gate[part] * projected_ref[part, :]
        joined_ref[part, :] = joined.astype(bf16)
        copy = pltpu.make_async_copy(joined_ref.at[part, :], out_ref.at[part, :], sems.at[k])
        copy.start()
        copies.append(copy)
    for copy in copies:
        copy.wait()


def local(hidden, hash_rows, memory_table, key_weight, value_weight, hidden_gain, key_gain):
    groups = lax.axis_size("dp")
    tensor = lax.axis_size("tensor")
    devices = groups * tensor
    rows_held, row_width = memory_table.shape
    shape = jax.ShapeDtypeStruct

    here = lax.axis_index(BOTH).astype(jnp.int32).reshape(1)
    hash_rows, here, hidden_gain, key_gain = lax.optimization_barrier((hash_rows, here, hidden_gain, key_gain))
    table_there = lax.ppermute(memory_table, "tensor", [(k, k ^ 1) for k in range(tensor)])
    chips = devices // 2
    message = call(
        lambda *refs: request_kernel(rows_held, *refs),
        shape((4 * chips, LANES), bf16),
        [hash_rows.reshape(1, LANES)],
        4 * MIB,
        flops=COVER,
    )
    in_turn = [[2 * chip + core for chip in chip_order()] for core in range(2)]
    in_place = [[2 * chip + core for chip in range(chips)] for core in range(2)]
    asked = lax.all_to_all(
        message.reshape(chips, 4, LANES), BOTH, 0, 0, axis_index_groups=in_place, tiled=True
    ).reshape(4 * chips, LANES)
    sent = call(
        gather_kernel,
        shape((8 * chips, row_width), bf16),
        [asked, memory_table, table_there],
        6 * MIB,
        scalars=[here],
        flops=COVER // 2,
    )
    arrived = lax.all_to_all(
        sent.reshape(chips, 8, row_width), BOTH, 0, 0, axis_index_groups=in_turn, tiled=True
    ).reshape(8 * chips, row_width)
    mine = call(place_kernel, shape((LANES, 2 * row_width), bf16), [asked, arrived], 6 * MIB, scalars=[here])
    other = lax.ppermute(mine, "tensor", [(k, k ^ 1) for k in range(tensor)])
    columns = key_weight.shape[1]
    work = 2 * LANES * 2 * row_width * columns
    key_weight = pltpu.with_memory_space_constraint(key_weight, pltpu.VMEM)
    value_weight = pltpu.with_memory_space_constraint(value_weight, pltpu.VMEM)
    partial = shape((LANES, columns), f32)
    key = call(
        own_key_kernel, partial, [mine, key_weight, value_weight], 6 * MIB, scalars=[here], flops=work
    )
    sums = call(
        key_kernel,
        shape((8, LANES), f32),
        [other, key_weight, key, hidden, hidden_gain.reshape(1, columns), key_gain.reshape(1, columns)],
        6 * MIB,
        scalars=[here],
        flops=work,
    )
    others = [lax.ppermute(sums, "tensor", [(k, k ^ d) for k in range(tensor)]) for d in (3, 2, 1)]
    projected = call(value_kernel, partial, [mine, other, value_weight], 6 * MIB, scalars=[here], flops=2 * work)
    chunks = 4
    return pl.pallas_call(
        lambda *refs: join_kernel(chunks, *refs),
        out_shape=shape(hidden.shape, bf16),
        in_specs=vmem(6),
        out_specs=pl.BlockSpec(memory_space=pl.ANY),
        scratch_shapes=[pltpu.VMEM(hidden.shape, bf16), pltpu.SemaphoreType.DMA((chunks,))],
        compiler_params=pltpu.CompilerParams(vmem_limit_bytes=6 * MIB),
    )(sums, *others, hidden, projected)


def solution(mesh):
    return jax.shard_map(
        local,
        mesh=mesh,
        in_specs=(
            P("dp", "tensor"),
            P("dp", "tensor"),
            P(("dp", "tensor"), None),
            P(None, "tensor"),
            P(None, "tensor"),
            P("tensor"),
            P("tensor"),
        ),
        out_specs=P("dp", "tensor"),
        check_vma=False,
    )
```

```python
import math

import jax
import jax.numpy as jnp
from jax import lax
from jax.experimental import pallas as pl
from jax.experimental.pallas import tpu as pltpu
from jax.sharding import PartitionSpec as P

D = 7168
LANES = 128
EPSILON = 1e-06
COVER = 20_000_000_000
BOTH = ("dp", "tensor")
MIB = 1024 * 1024

f32 = jnp.float32
bf16 = jnp.bfloat16


def iota(shape, dim):
    return lax.broadcasted_iota(jnp.int32, shape, dim)


def vmem(count):
    return [pl.BlockSpec(memory_space=pltpu.VMEM)] * count


def call(body, out_shape, inputs, limit, scalars=(), scratch=(), flops=0):
    many = isinstance(out_shape, (tuple, list))
    return pl.pallas_call(
        body,
        out_shape=out_shape,
        in_specs=[pl.BlockSpec(memory_space=pltpu.SMEM)] * len(scalars) + vmem(len(inputs)),
        out_specs=tuple(vmem(len(out_shape))) if many else vmem(1)[0],
        scratch_shapes=list(scratch),
        compiler_params=pltpu.CompilerParams(vmem_limit_bytes=limit),
        cost_estimate=pl.CostEstimate(flops=flops, transcendentals=0, bytes_accessed=0) if flops else None,
    )(*scalars, *inputs)


def request_kernel(rows_held, which, here_ref, hash_ref, *refs):
    *before, out_ref, row_ref, sem = refs
    half = here_ref[0] >> 6

    @pl.when(half == which)
    def _():
        copy = pltpu.make_async_copy(hash_ref, row_ref, sem)
        copy.start()
        copy.wait()
        row = row_ref[...]
        owner = row // rows_held
        local = (row - owner * rows_held).astype(f32)
        owner_rows = jnp.broadcast_to(owner.astype(f32), (LANES, LANES))
        owner_cols = owner_rows.T
        earlier = (owner_rows == owner_cols) & (iota((LANES, LANES), 0) < iota((LANES, LANES), 1))
        slot = jnp.sum(earlier.astype(f32), axis=0, keepdims=True).astype(jnp.int32)
        z = owner >> 5
        near = (z >> 1) == half
        server = (jnp.where(near, z, 3 - z) & 1) * 32 + (owner & 31)
        landing = server * 4 + jnp.where(near, slot, slot + 2)
        rows = out_ref.shape[0]
        asks = jnp.where(landing == iota((rows, LANES), 0), local, jnp.zeros((rows, LANES), f32))
        asks = jnp.sum(asks, axis=1, keepdims=True)
        where = landing.astype(f32)
        turned = pltpu.roll(where, LANES // 2, 1)
        first = (iota((rows, LANES), 0) & 3) == 0
        message = jnp.where(iota((rows, LANES), 1) < LANES // 2, asks, jnp.where(first, turned, where))
        out_ref[...] = message.astype(bf16)

    for ref in before:

        @pl.when(half != which)
        def _():
            out_ref[...] = ref[...]


def gather_kernel(asked_ref, mine_ref, other_ref, out_ref):
    index = asked_ref[...].astype(jnp.int32)[:, 0:1]
    rows = index.shape[0]
    held = mine_ref.shape[0]
    index = jnp.where(((iota((rows, 1), 0) >> 1) & 1) == 0, index, index + held)
    chosen = (index == iota((rows, 2 * held), 1)).astype(f32).astype(bf16)
    table = jnp.concatenate([mine_ref[...], other_ref[...]], axis=0)
    found = jnp.dot(chosen, table, preferred_element_type=f32).astype(bf16)
    both = [found[start : start + 16] for start in range(0, rows, 16) for _ in range(2)]
    out_ref[...] = jnp.concatenate(both, axis=0)


def place_kernel(heads, here_ref, asked_ref, arrived_ref, out_ref):
    core = here_ref[0] & 1
    start = pl.multiple_of(((here_ref[0] >> 2) & 15) * 16, 16)
    asked = asked_ref[pl.ds(start, 16), :].astype(f32)
    arrived = arrived_ref[...]
    slots = arrived.shape[0]
    width = arrived.shape[1]
    low = iota((1, LANES), 1) < LANES // 2
    turned = pltpu.roll(asked, LANES // 2, 1)
    for k, head in enumerate(heads):
        landing = jnp.where(low, turned[4 * head : 4 * head + 1], asked[4 * head + 1 : 4 * head + 2])
        landing = landing.astype(jnp.int32)
        target = (landing >> 3) * 16 + head * 4 + (landing & 3)
        target = jnp.where(((landing >> 2) & 1) == core, target, -1)
        chosen = (target == iota((slots, LANES), 0)).astype(f32).astype(bf16)
        found = lax.dot_general(chosen, arrived, (((0,), (0,)), ((), ())), preferred_element_type=f32)
        out_ref[:, k * width : (k + 1) * width] = found.astype(bf16)


def row_of_sums(terms):
    parts = terms[:, 0:LANES]
    for k in range(1, terms.shape[1] // LANES):
        parts = parts + terms[:, k * LANES : (k + 1) * LANES]
    return jnp.sum(parts.T, axis=0, keepdims=True)


def first_kernel(mine_ref, other_ref, weight_ref, _, out_ref):
    memory = mine_ref[...] + other_ref[...]
    out_ref[...] = jnp.dot(memory, weight_ref[: memory.shape[1], :], preferred_element_type=f32)


def value_kernel(mine0_ref, other0_ref, mine1_ref, other1_ref, weight_ref, out_ref):
    memory = jnp.concatenate([mine0_ref[...] + other0_ref[...], mine1_ref[...] + other1_ref[...]], axis=1)
    out_ref[...] = jnp.dot(memory, weight_ref[...], preferred_element_type=f32)


def key_kernel(mine_ref, other_ref, weight_ref, first_ref, hidden_ref, hgain_ref, kgain_ref, sums_ref):
    memory = mine_ref[...] + other_ref[...]
    key = first_ref[...] + jnp.dot(memory, weight_ref[memory.shape[1] :, :], preferred_element_type=f32)
    hidden = hidden_ref[...].astype(f32)
    sums = [
        row_of_sums(hidden * hidden),
        row_of_sums(key * key),
        row_of_sums((hidden * hgain_ref[...]) * (key * kgain_ref[...])),
    ]
    sums_ref[...] = jnp.concatenate(sums + [jnp.zeros((5, LANES), f32)], axis=0)


def join_kernel(chunks, s0_ref, s1_ref, s2_ref, s3_ref, hidden_ref, projected_ref, out_ref, joined_ref, sems):
    sums = (s0_ref[...] + s1_ref[...]) + (s2_ref[...] + s3_ref[...])
    hidden_power = sums[0:1] / D
    key_power = sums[1:2] / D
    agreement = sums[2:3] * lax.rsqrt(hidden_power + EPSILON) * lax.rsqrt(key_power + EPSILON)
    gate = jax.nn.sigmoid(agreement / math.sqrt(D))
    gate = jnp.broadcast_to(gate, (LANES, LANES)).T[:, 0:1]
    rows = LANES // chunks
    copies = []
    for k in range(chunks):
        part = slice(k * rows, (k + 1) * rows)
        joined = hidden_ref[part, :].astype(f32) + gate[part] * projected_ref[part, :]
        joined_ref[part, :] = joined.astype(bf16)
        copy = pltpu.make_async_copy(joined_ref.at[part, :], out_ref.at[part, :], sems.at[k])
        copy.start()
        copies.append(copy)
    for copy in copies:
        copy.wait()


def local(hidden, hash_rows, memory_table, key_weight, value_weight, hidden_gain, key_gain):
    groups = lax.axis_size("dp")
    tensor = lax.axis_size("tensor")
    devices = groups * tensor
    rows_held, row_width = memory_table.shape
    shape = jax.ShapeDtypeStruct

    here = lax.axis_index(BOTH).astype(jnp.int32).reshape(1)
    hash_rows, here, hidden_gain, key_gain = lax.optimization_barrier((hash_rows, here, hidden_gain, key_gain))
    servers = devices // 2
    rows = pltpu.with_memory_space_constraint(hash_rows.reshape(1, LANES), pltpu.HBM)

    def request(which, *before):
        return pl.pallas_call(
            lambda *refs: request_kernel(rows_held, which, *refs),
            out_shape=shape((4 * servers, LANES), bf16),
            in_specs=[pl.BlockSpec(memory_space=pltpu.SMEM), pl.BlockSpec(memory_space=pltpu.HBM)] + vmem(len(before)),
            out_specs=vmem(1)[0],
            scratch_shapes=[pltpu.VMEM((1, LANES), jnp.int32), pltpu.SemaphoreType.DMA(())],
            compiler_params=pltpu.CompilerParams(vmem_limit_bytes=2 * MIB),
            cost_estimate=pl.CostEstimate(flops=COVER if before else 1, transcendentals=0, bytes_accessed=1),
        )(here, rows, *before)

    message = request(0)
    message, memory_table = lax.optimization_barrier((message, memory_table))
    swap = [(k, (3 - (k >> 5)) * 32 + (k & 31)) for k in range(devices)]
    table_there = lax.ppermute(memory_table, BOTH, swap)
    message = request(1, message)
    halves_of_z = [[half * servers + k for k in range(servers)] for half in range(2)]
    same_core = [[k for k in half if k % 2 == core] for half in halves_of_z for core in range(2)]
    asked = lax.all_to_all(
        message.reshape(servers, 4, LANES), BOTH, 0, 0, axis_index_groups=halves_of_z, tiled=True
    ).reshape(4 * servers, LANES)
    sent = call(
        gather_kernel,
        shape((8 * servers, row_width), bf16),
        [asked, memory_table, table_there],
        6 * MIB,
        flops=14_000_000_000,
    )
    arrived = lax.all_to_all(
        sent.reshape(servers // 2, 16, row_width), BOTH, 0, 0, axis_index_groups=same_core, tiled=True
    ).reshape(8 * servers, row_width)
    halves = []
    for heads in ((0, 1), (2, 3)):
        mine = call(
            lambda *refs, heads=heads: place_kernel(heads, *refs),
            shape((LANES, 2 * row_width), bf16),
            [asked, arrived],
            6 * MIB,
            scalars=[here],
        )
        halves.append((mine, lax.ppermute(mine, "tensor", [(k, k ^ 1) for k in range(tensor)])))
    columns = key_weight.shape[1]
    work = 2 * LANES * 2 * row_width * columns
    key_weight = pltpu.with_memory_space_constraint(key_weight, pltpu.VMEM)
    value_weight = pltpu.with_memory_space_constraint(value_weight, pltpu.VMEM)
    partial = shape((LANES, columns), f32)
    key = call(first_kernel, partial, [*halves[0], key_weight, value_weight], 6 * MIB, flops=work)
    sums = call(
        key_kernel,
        shape((8, LANES), f32),
        [*halves[1], key_weight, key, hidden, hidden_gain.reshape(1, columns), key_gain.reshape(1, columns)],
        6 * MIB,
        flops=work,
    )
    others = [lax.ppermute(sums, "tensor", [(k, k ^ d) for k in range(tensor)]) for d in (3, 2, 1)]
    projected = call(value_kernel, partial, [*halves[0], *halves[1], value_weight], 6 * MIB, flops=2 * work)
    chunks = 4
    return pl.pallas_call(
        lambda *refs: join_kernel(chunks, *refs),
        out_shape=shape(hidden.shape, bf16),
        in_specs=vmem(6),
        out_specs=pl.BlockSpec(memory_space=pl.ANY),
        scratch_shapes=[pltpu.VMEM(hidden.shape, bf16), pltpu.SemaphoreType.DMA((chunks,))],
        compiler_params=pltpu.CompilerParams(vmem_limit_bytes=6 * MIB),
    )(sums, *others, hidden, projected)


def solution(mesh):
    return jax.shard_map(
        local,
        mesh=mesh,
        in_specs=(
            P("dp", "tensor"),
            P("dp", "tensor"),
            P(("dp", "tensor"), None),
            P(None, "tensor"),
            P(None, "tensor"),
            P("tensor"),
            P("tensor"),
        ),
        out_specs=P("dp", "tensor"),
        check_vma=False,
    )
```

```python
import math

import jax
import jax.numpy as jnp
from jax import lax
from jax.experimental import pallas as pl
from jax.experimental.pallas import tpu as pltpu
from jax.sharding import PartitionSpec as P

D = 7168
LANES = 128
EPSILON = 1e-06
COVER = 20_000_000_000
BOTH = ("dp", "tensor")
MIB = 1024 * 1024

f32 = jnp.float32
bf16 = jnp.bfloat16


def group_order():
    order = []
    for k in range(16):
        e, p, q = k & 1, (k >> 1) & 1, k >> 2
        order.append((p ^ e) * 8 + ((q + 2 * e) & 3) * 2 + e)
    return order


def turn_of(group):
    z, y, e = group >> 3, (group >> 1) & 3, group & 1
    return e + (z ^ e) * 2 + ((y - 2 * e) & 3) * 4


def iota(shape, dim):
    return lax.broadcasted_iota(jnp.int32, shape, dim)


def vmem(count):
    return [pl.BlockSpec(memory_space=pltpu.VMEM)] * count


def call(body, out_shape, inputs, limit, scalars=(), scratch=(), flops=0):
    many = isinstance(out_shape, (tuple, list))
    return pl.pallas_call(
        body,
        out_shape=out_shape,
        in_specs=[pl.BlockSpec(memory_space=pltpu.SMEM)] * len(scalars) + vmem(len(inputs)),
        out_specs=tuple(vmem(len(out_shape))) if many else vmem(1)[0],
        scratch_shapes=list(scratch),
        compiler_params=pltpu.CompilerParams(vmem_limit_bytes=limit),
        cost_estimate=pl.CostEstimate(flops=flops, transcendentals=0, bytes_accessed=0) if flops else None,
    )(*scalars, *inputs)


def request_kernel(rows_held, which, here_ref, hash_ref, *refs):
    *before, out_ref, row_ref, sem = refs
    half = here_ref[0] >> 6

    @pl.when(half == which)
    def _():
        copy = pltpu.make_async_copy(hash_ref, row_ref, sem)
        copy.start()
        copy.wait()
        row = row_ref[...]
        owner = row // rows_held
        local = (row - owner * rows_held).astype(f32)
        owner_rows = jnp.broadcast_to(owner.astype(f32), (LANES, LANES))
        owner_cols = owner_rows.T
        earlier = (owner_rows == owner_cols) & (iota((LANES, LANES), 0) < iota((LANES, LANES), 1))
        slot = jnp.sum(earlier.astype(f32), axis=0, keepdims=True).astype(jnp.int32)
        z = owner >> 5
        near = (z >> 1) == half
        server = (jnp.where(near, z, 3 - z) & 1) * 32 + (owner & 31)
        landing = server * 4 + jnp.where(near, slot, slot + 2)
        rows = out_ref.shape[0]
        place = turn_of(server >> 2) * 16 + (landing & 15)
        asks = jnp.where(place == iota((rows, LANES), 0), local, jnp.zeros((rows, LANES), f32))
        asks = jnp.sum(asks, axis=1, keepdims=True)
        where = landing.astype(f32)
        turned = pltpu.roll(where, LANES // 2, 1)
        first = (iota((rows, LANES), 0) & 3) == 0
        message = jnp.where(iota((rows, LANES), 1) < LANES // 2, asks, jnp.where(first, turned, where))
        out_ref[...] = message.astype(bf16)

    for ref in before:

        @pl.when(half != which)
        def _():
            out_ref[...] = ref[...]


def gather_kernel(asked_ref, mine_ref, other_ref, out_ref):
    index = asked_ref[...].astype(jnp.int32)[:, 0:1]
    rows = index.shape[0]
    held = mine_ref.shape[0]
    index = jnp.where(((iota((rows, 1), 0) >> 1) & 1) == 0, index, index + held)
    chosen = (index == iota((rows, 2 * held), 1)).astype(f32).astype(bf16)
    table = jnp.concatenate([mine_ref[...], other_ref[...]], axis=0)
    found = jnp.dot(chosen, table, preferred_element_type=f32).astype(bf16)
    starts = [turn_of(chip // 2) * 16 for chip in range(rows // 8)]
    both = [found[start : start + 16] for start in starts]
    out_ref[...] = jnp.concatenate(both, axis=0)


def place_kernel(heads, here_ref, asked_ref, arrived_ref, out_ref):
    core = here_ref[0] & 1
    start = pl.multiple_of(turn_of((here_ref[0] >> 2) & 15) * 16, 16)
    asked = asked_ref[pl.ds(start, 16), :].astype(f32)
    arrived = arrived_ref[...]
    slots = arrived.shape[0]
    width = arrived.shape[1]
    low = iota((1, LANES), 1) < LANES // 2
    turned = pltpu.roll(asked, LANES // 2, 1)
    for k, head in enumerate(heads):
        landing = jnp.where(low, turned[4 * head : 4 * head + 1], asked[4 * head + 1 : 4 * head + 2])
        landing = landing.astype(jnp.int32)
        target = (landing >> 3) * 16 + head * 4 + (landing & 3)
        target = jnp.where(((landing >> 2) & 1) == core, target, -1)
        chosen = (target == iota((slots, LANES), 0)).astype(f32).astype(bf16)
        found = lax.dot_general(chosen, arrived, (((0,), (0,)), ((), ())), preferred_element_type=f32)
        out_ref[:, k * width : (k + 1) * width] = found.astype(bf16)


def row_of_sums(terms):
    parts = terms[:, 0:LANES]
    for k in range(1, terms.shape[1] // LANES):
        parts = parts + terms[:, k * LANES : (k + 1) * LANES]
    return jnp.sum(parts.T, axis=0, keepdims=True)


def first_kernel(mine_ref, other_ref, weight_ref, _, out_ref):
    memory = mine_ref[...] + other_ref[...]
    out_ref[...] = jnp.dot(memory, weight_ref[: memory.shape[1], :], preferred_element_type=f32)


def value_kernel(mine0_ref, other0_ref, mine1_ref, other1_ref, weight_ref, out_ref):
    memory = jnp.concatenate([mine0_ref[...] + other0_ref[...], mine1_ref[...] + other1_ref[...]], axis=1)
    out_ref[...] = jnp.dot(memory, weight_ref[...], preferred_element_type=f32)


def key_kernel(mine_ref, other_ref, weight_ref, first_ref, hidden_ref, hgain_ref, kgain_ref, sums_ref):
    memory = mine_ref[...] + other_ref[...]
    key = first_ref[...] + jnp.dot(memory, weight_ref[memory.shape[1] :, :], preferred_element_type=f32)
    hidden = hidden_ref[...].astype(f32)
    sums = [
        row_of_sums(hidden * hidden),
        row_of_sums(key * key),
        row_of_sums((hidden * hgain_ref[...]) * (key * kgain_ref[...])),
    ]
    sums_ref[...] = jnp.concatenate(sums + [jnp.zeros((5, LANES), f32)], axis=0)


def join_kernel(chunks, s0_ref, s1_ref, s2_ref, s3_ref, hidden_ref, projected_ref, out_ref, joined_ref, sems):
    sums = (s0_ref[...] + s1_ref[...]) + (s2_ref[...] + s3_ref[...])
    hidden_power = sums[0:1] / D
    key_power = sums[1:2] / D
    agreement = sums[2:3] * lax.rsqrt(hidden_power + EPSILON) * lax.rsqrt(key_power + EPSILON)
    gate = jax.nn.sigmoid(agreement / math.sqrt(D))
    gate = jnp.broadcast_to(gate, (LANES, LANES)).T
    rows = LANES // chunks
    copies = []
    for k in range(chunks):
        part = slice(k * rows, (k + 1) * rows)
        for column in range(0, joined_ref.shape[1], LANES):
            lanes = slice(column, column + LANES)
            joined = hidden_ref[part, lanes].astype(f32) + gate[part] * projected_ref[part, lanes]
            joined_ref[part, lanes] = joined.astype(bf16)
        copy = pltpu.make_async_copy(joined_ref.at[part, :], out_ref.at[part, :], sems.at[k])
        copy.start()
        copies.append(copy)
    for copy in copies:
        copy.wait()


def local(hidden, hash_rows, memory_table, key_weight, value_weight, hidden_gain, key_gain):
    groups = lax.axis_size("dp")
    tensor = lax.axis_size("tensor")
    devices = groups * tensor
    rows_held, row_width = memory_table.shape
    shape = jax.ShapeDtypeStruct

    here = lax.axis_index(BOTH).astype(jnp.int32).reshape(1)
    hash_rows, here, hidden_gain, key_gain = lax.optimization_barrier((hash_rows, here, hidden_gain, key_gain))
    servers = devices // 2
    rows = pltpu.with_memory_space_constraint(hash_rows.reshape(1, LANES), pltpu.HBM)

    def request(which, *before):
        return pl.pallas_call(
            lambda *refs: request_kernel(rows_held, which, *refs),
            out_shape=shape((4 * servers, LANES), bf16),
            in_specs=[pl.BlockSpec(memory_space=pltpu.SMEM), pl.BlockSpec(memory_space=pltpu.HBM)] + vmem(len(before)),
            out_specs=vmem(1)[0],
            scratch_shapes=[pltpu.VMEM((1, LANES), jnp.int32), pltpu.SemaphoreType.DMA(())],
            compiler_params=pltpu.CompilerParams(vmem_limit_bytes=2 * MIB),
            cost_estimate=pl.CostEstimate(flops=COVER if before else 1, transcendentals=0, bytes_accessed=1),
        )(here, rows, *before)

    message = request(0)
    message, memory_table = lax.optimization_barrier((message, memory_table))
    swap = [(k, (3 - (k >> 5)) * 32 + (k & 31)) for k in range(devices)]
    table_there = lax.ppermute(memory_table, BOTH, swap)
    message = request(1, message)
    halves_of_z = [[half * servers + k for k in range(servers)] for half in range(2)]
    same_core = [[k for k in half if k % 2 == core] for half in halves_of_z for core in range(2)]
    by_group = [[half[4 * group + k] for group in group_order() for k in range(4)] for half in halves_of_z]
    asked = lax.all_to_all(
        message.reshape(servers, 4, LANES), BOTH, 0, 0, axis_index_groups=by_group, tiled=True
    ).reshape(4 * servers, LANES)
    sent = call(
        gather_kernel,
        shape((8 * servers, row_width), bf16),
        [asked, memory_table, table_there],
        6 * MIB,
        flops=COVER // 2,
    )
    arrived = lax.all_to_all(
        sent.reshape(servers // 2, 16, row_width), BOTH, 0, 0, axis_index_groups=same_core, tiled=True
    ).reshape(8 * servers, row_width)
    halves = []
    for heads in ((0, 1), (2, 3)):
        mine = call(
            lambda *refs, heads=heads: place_kernel(heads, *refs),
            shape((LANES, 2 * row_width), bf16),
            [asked, arrived],
            6 * MIB,
            scalars=[here],
        )
        halves.append((mine, lax.ppermute(mine, "tensor", [(k, k ^ 1) for k in range(tensor)])))
    columns = key_weight.shape[1]
    work = 2 * LANES * 2 * row_width * columns
    key_weight = pltpu.with_memory_space_constraint(key_weight, pltpu.VMEM)
    value_weight = pltpu.with_memory_space_constraint(value_weight, pltpu.VMEM)
    partial = shape((LANES, columns), f32)
    key = call(first_kernel, partial, [*halves[0], key_weight, value_weight], 6 * MIB, flops=work)
    sums = call(
        key_kernel,
        shape((8, LANES), f32),
        [*halves[1], key_weight, key, hidden, hidden_gain.reshape(1, columns), key_gain.reshape(1, columns)],
        6 * MIB,
        flops=work,
    )
    others = [lax.ppermute(sums, "tensor", [(k, k ^ d) for k in range(tensor)]) for d in (3, 2, 1)]
    projected = call(value_kernel, partial, [*halves[0], *halves[1], value_weight], 6 * MIB, flops=2 * work)
    chunks = 4
    return pl.pallas_call(
        lambda *refs: join_kernel(chunks, *refs),
        out_shape=shape(hidden.shape, bf16),
        in_specs=vmem(6),
        out_specs=pl.BlockSpec(memory_space=pl.ANY),
        scratch_shapes=[pltpu.VMEM(hidden.shape, bf16), pltpu.SemaphoreType.DMA((chunks,))],
        compiler_params=pltpu.CompilerParams(vmem_limit_bytes=6 * MIB),
    )(sums, *others, hidden, projected)


def solution(mesh):
    return jax.shard_map(
        local,
        mesh=mesh,
        in_specs=(
            P("dp", "tensor"),
            P("dp", "tensor"),
            P(("dp", "tensor"), None),
            P(None, "tensor"),
            P(None, "tensor"),
            P("tensor"),
            P("tensor"),
        ),
        out_specs=P("dp", "tensor"),
        check_vma=False,
    )
```

```python
import math

import jax
import jax.numpy as jnp
from jax import lax
from jax.experimental import pallas as pl
from jax.experimental.pallas import tpu as pltpu
from jax.sharding import PartitionSpec as P

D = 7168
LANES = 128
EPSILON = 1e-06
COVER = 20_000_000_000
BOTH = ("dp", "tensor")
MIB = 1024 * 1024

f32 = jnp.float32
bf16 = jnp.bfloat16


def group_order():
    order = []
    for k in range(16):
        e, p, q = k & 1, (k >> 1) & 1, k >> 2
        order.append((p ^ e) * 8 + ((q + 2 * e) & 3) * 2 + e)
    return order


def turn_of(group):
    z, y, e = group >> 3, (group >> 1) & 3, group & 1
    return e + (z ^ e) * 2 + ((y - 2 * e) & 3) * 4


def iota(shape, dim):
    return lax.broadcasted_iota(jnp.int32, shape, dim)


def vmem(count):
    return [pl.BlockSpec(memory_space=pltpu.VMEM)] * count


def call(body, out_shape, inputs, limit, scalars=(), scratch=(), flops=0):
    many = isinstance(out_shape, (tuple, list))
    return pl.pallas_call(
        body,
        out_shape=out_shape,
        in_specs=[pl.BlockSpec(memory_space=pltpu.SMEM)] * len(scalars) + vmem(len(inputs)),
        out_specs=tuple(vmem(len(out_shape))) if many else vmem(1)[0],
        scratch_shapes=list(scratch),
        compiler_params=pltpu.CompilerParams(vmem_limit_bytes=limit),
        cost_estimate=pl.CostEstimate(flops=flops, transcendentals=0, bytes_accessed=0) if flops else None,
    )(*scalars, *inputs)


def request_kernel(rows_held, which, here_ref, hash_ref, *refs):
    *before, out_ref, row_ref, sem = refs
    half = here_ref[0] >> 6

    @pl.when(half == which)
    def _():
        copy = pltpu.make_async_copy(hash_ref, row_ref, sem)
        copy.start()
        copy.wait()
        row = row_ref[...]
        owner = row // rows_held
        local = (row - owner * rows_held).astype(f32)
        owner_rows = jnp.broadcast_to(owner.astype(f32), (LANES, LANES))
        owner_cols = owner_rows.T
        earlier = (owner_rows == owner_cols) & (iota((LANES, LANES), 0) < iota((LANES, LANES), 1))
        slot = jnp.sum(earlier.astype(f32), axis=0, keepdims=True).astype(jnp.int32)
        z = owner >> 5
        near = (z >> 1) == half
        server = (jnp.where(near, z, 3 - z) & 1) * 32 + (owner & 31)
        landing = server * 4 + jnp.where(near, slot, slot + 2)
        rows = out_ref.shape[0]
        place = turn_of(server >> 2) * 16 + (landing & 15)
        asks = jnp.where(place == iota((rows, LANES), 0), local, jnp.zeros((rows, LANES), f32))
        asks = jnp.sum(asks, axis=1, keepdims=True)
        where = landing.astype(f32)
        turned = pltpu.roll(where, LANES // 2, 1)
        first = (iota((rows, LANES), 0) & 3) == 0
        message = jnp.where(iota((rows, LANES), 1) < LANES // 2, asks, jnp.where(first, turned, where))
        out_ref[...] = message.astype(bf16)

    for ref in before:

        @pl.when(half != which)
        def _():
            out_ref[...] = ref[...]


def gather_kernel(asked_ref, mine_ref, other_ref, out_ref):
    index = asked_ref[...].astype(jnp.int32)[:, 0:1]
    rows = index.shape[0]
    held = mine_ref.shape[0]
    index = jnp.where(((iota((rows, 1), 0) >> 1) & 1) == 0, index, index + held)
    chosen = (index == iota((rows, 2 * held), 1)).astype(f32).astype(bf16)
    table = jnp.concatenate([mine_ref[...], other_ref[...]], axis=0)
    found = jnp.dot(chosen, table, preferred_element_type=f32).astype(bf16)
    starts = [turn_of(chip // 2) * 16 for chip in range(rows // 8)]
    both = [found[start : start + 16] for start in starts]
    out_ref[...] = jnp.concatenate(both, axis=0)


def place_kernel(heads, here_ref, asked_ref, arrived_ref, out_ref):
    core = here_ref[0] & 1
    start = pl.multiple_of(turn_of((here_ref[0] >> 2) & 15) * 16, 16)
    asked = asked_ref[pl.ds(start, 16), :].astype(f32)
    arrived = arrived_ref[...]
    slots = arrived.shape[0]
    width = arrived.shape[1]
    low = iota((1, LANES), 1) < LANES // 2
    turned = pltpu.roll(asked, LANES // 2, 1)
    for k, head in enumerate(heads):
        landing = jnp.where(low, turned[4 * head : 4 * head + 1], asked[4 * head + 1 : 4 * head + 2])
        landing = landing.astype(jnp.int32)
        target = (landing >> 3) * 16 + head * 4 + (landing & 3)
        target = jnp.where(((landing >> 2) & 1) == core, target, -1)
        chosen = (target == iota((slots, LANES), 0)).astype(f32).astype(bf16)
        found = lax.dot_general(chosen, arrived, (((0,), (0,)), ((), ())), preferred_element_type=f32)
        out_ref[:, k * width : (k + 1) * width] = found.astype(bf16)


def row_of_sums(terms):
    parts = terms[:, 0:LANES]
    for k in range(1, terms.shape[1] // LANES):
        parts = parts + terms[:, k * LANES : (k + 1) * LANES]
    return jnp.sum(parts.T, axis=0, keepdims=True)


def first_kernel(mine_ref, other_ref, weight_ref, _, out_ref):
    memory = mine_ref[...] + other_ref[...]
    out_ref[...] = jnp.dot(memory, weight_ref[: memory.shape[1], :], preferred_element_type=f32)


def value_kernel(mine0_ref, other0_ref, mine1_ref, other1_ref, weight_ref, out_ref):
    memory = jnp.concatenate([mine0_ref[...] + other0_ref[...], mine1_ref[...] + other1_ref[...]], axis=1)
    out_ref[...] = jnp.dot(memory, weight_ref[...], preferred_element_type=f32)


def key_kernel(mine_ref, other_ref, weight_ref, first_ref, hidden_ref, hgain_ref, kgain_ref, sums_ref):
    memory = mine_ref[...] + other_ref[...]
    key = first_ref[...] + jnp.dot(memory, weight_ref[memory.shape[1] :, :], preferred_element_type=f32)
    hidden = hidden_ref[...].astype(f32)
    sums = [
        row_of_sums(hidden * hidden),
        row_of_sums(key * key),
        row_of_sums((hidden * hgain_ref[...]) * (key * kgain_ref[...])),
    ]
    sums_ref[...] = jnp.concatenate(sums + [jnp.zeros((5, LANES), f32)], axis=0)


def join_kernel(chunks, s0_ref, s1_ref, s2_ref, s3_ref, hidden_ref, projected_ref, out_ref, joined_ref, sems):
    sums = (s0_ref[...] + s1_ref[...]) + (s2_ref[...] + s3_ref[...])
    hidden_power = sums[0:1] / D
    key_power = sums[1:2] / D
    agreement = sums[2:3] * lax.rsqrt(hidden_power + EPSILON) * lax.rsqrt(key_power + EPSILON)
    gate = jax.nn.sigmoid(agreement / math.sqrt(D))
    gate = jnp.broadcast_to(gate, (LANES, LANES)).T
    rows = LANES // chunks
    copies = []
    for k in range(chunks):
        part = slice(k * rows, (k + 1) * rows)
        for column in range(0, joined_ref.shape[1], LANES):
            lanes = slice(column, column + LANES)
            joined = hidden_ref[part, lanes].astype(f32) + gate[part] * projected_ref[part, lanes]
            joined_ref[part, lanes] = joined.astype(bf16)
        copy = pltpu.make_async_copy(joined_ref.at[part, :], out_ref.at[part, :], sems.at[k])
        copy.start()
        copies.append(copy)
    for copy in copies:
        copy.wait()


def local(hidden, hash_rows, memory_table, key_weight, value_weight, hidden_gain, key_gain):
    groups = lax.axis_size("dp")
    tensor = lax.axis_size("tensor")
    devices = groups * tensor
    rows_held, row_width = memory_table.shape
    shape = jax.ShapeDtypeStruct

    here = lax.axis_index(BOTH).astype(jnp.int32).reshape(1)
    hash_rows, here, hidden_gain, key_gain = lax.optimization_barrier((hash_rows, here, hidden_gain, key_gain))
    servers = devices // 2
    rows = pltpu.with_memory_space_constraint(hash_rows.reshape(1, LANES), pltpu.HBM)

    def request(which, *before):
        return pl.pallas_call(
            lambda *refs: request_kernel(rows_held, which, *refs),
            out_shape=shape((4 * servers, LANES), bf16),
            in_specs=[pl.BlockSpec(memory_space=pltpu.SMEM), pl.BlockSpec(memory_space=pltpu.HBM)] + vmem(len(before)),
            out_specs=vmem(1)[0],
            scratch_shapes=[pltpu.VMEM((1, LANES), jnp.int32), pltpu.SemaphoreType.DMA(())],
            compiler_params=pltpu.CompilerParams(vmem_limit_bytes=2 * MIB),
            cost_estimate=pl.CostEstimate(flops=COVER if before else 1, transcendentals=0, bytes_accessed=1),
        )(here, rows, *before)

    message = request(0)
    message, memory_table = lax.optimization_barrier((message, memory_table))
    swap = [(k, (3 - (k >> 5)) * 32 + (k & 31)) for k in range(devices)]
    table_there = lax.ppermute(memory_table, BOTH, swap)
    message = request(1, message)
    halves_of_z = [[half * servers + k for k in range(servers)] for half in range(2)]
    same_core = [[k for k in half if k % 2 == core] for half in halves_of_z for core in range(2)]
    by_group = [[half[4 * group + k] for group in group_order() for k in range(4)] for half in halves_of_z]
    asked = lax.all_to_all(
        message.reshape(servers, 4, LANES), BOTH, 0, 0, axis_index_groups=by_group, tiled=True
    ).reshape(4 * servers, LANES)
    sent = call(
        gather_kernel,
        shape((8 * servers, row_width), bf16),
        [asked, memory_table, table_there],
        6 * MIB,
        flops=COVER // 2,
    )
    arrived = lax.all_to_all(
        sent.reshape(servers // 2, 16, row_width), BOTH, 0, 0, axis_index_groups=same_core, tiled=True
    ).reshape(8 * servers, row_width)
    halves = []
    for heads in ((0, 1), (2, 3)):
        mine = call(
            lambda *refs, heads=heads: place_kernel(heads, *refs),
            shape((LANES, 2 * row_width), bf16),
            [asked, arrived],
            6 * MIB,
            scalars=[here],
        )
        halves.append((mine, lax.ppermute(mine, "tensor", [(k, k ^ 1) for k in range(tensor)])))
    columns = key_weight.shape[1]
    work = 2 * LANES * 2 * row_width * columns
    key_weight = pltpu.with_memory_space_constraint(key_weight, pltpu.VMEM)
    value_weight = pltpu.with_memory_space_constraint(value_weight, pltpu.VMEM)
    partial = shape((LANES, columns), f32)
    key = call(first_kernel, partial, [*halves[0], key_weight, value_weight], 6 * MIB, flops=work)
    sums = call(
        key_kernel,
        shape((8, LANES), f32),
        [*halves[1], key_weight, key, hidden, hidden_gain.reshape(1, columns), key_gain.reshape(1, columns)],
        6 * MIB,
        flops=work,
    )
    others = [lax.ppermute(sums, "tensor", [(k, k ^ d) for k in range(tensor)]) for d in (2, 3, 1)]
    projected = call(value_kernel, partial, [*halves[0], *halves[1], value_weight], 6 * MIB, flops=2 * work)
    chunks = 4
    return pl.pallas_call(
        lambda *refs: join_kernel(chunks, *refs),
        out_shape=shape(hidden.shape, bf16),
        in_specs=vmem(6),
        out_specs=pl.BlockSpec(memory_space=pl.ANY),
        scratch_shapes=[pltpu.VMEM(hidden.shape, bf16), pltpu.SemaphoreType.DMA((chunks,))],
        compiler_params=pltpu.CompilerParams(vmem_limit_bytes=6 * MIB),
    )(sums, *others, hidden, projected)


def solution(mesh):
    return jax.shard_map(
        local,
        mesh=mesh,
        in_specs=(
            P("dp", "tensor"),
            P("dp", "tensor"),
            P(("dp", "tensor"), None),
            P(None, "tensor"),
            P(None, "tensor"),
            P("tensor"),
            P("tensor"),
        ),
        out_specs=P("dp", "tensor"),
        check_vma=False,
    )
```

```python
import math

import jax
import jax.numpy as jnp
from jax import lax
from jax.experimental import pallas as pl
from jax.experimental.pallas import tpu as pltpu
from jax.sharding import PartitionSpec as P

D = 7168
LANES = 128
EPSILON = 1e-06
COVER = 20_000_000_000
BOTH = ("dp", "tensor")
MIB = 1024 * 1024

f32 = jnp.float32
bf16 = jnp.bfloat16


def group_order():
    order = []
    for k in range(16):
        e, p, q = k & 1, (k >> 1) & 1, k >> 2
        order.append((p ^ e) * 8 + ((q + 2 * e) & 3) * 2 + e)
    return order


def turn_of(group):
    z, y, e = group >> 3, (group >> 1) & 3, group & 1
    return e + (z ^ e) * 2 + ((y - 2 * e) & 3) * 4


def iota(shape, dim):
    return lax.broadcasted_iota(jnp.int32, shape, dim)


def vmem(count):
    return [pl.BlockSpec(memory_space=pltpu.VMEM)] * count


def call(body, out_shape, inputs, limit, scalars=(), scratch=(), flops=0):
    many = isinstance(out_shape, (tuple, list))
    return pl.pallas_call(
        body,
        out_shape=out_shape,
        in_specs=[pl.BlockSpec(memory_space=pltpu.SMEM)] * len(scalars) + vmem(len(inputs)),
        out_specs=tuple(vmem(len(out_shape))) if many else vmem(1)[0],
        scratch_shapes=list(scratch),
        compiler_params=pltpu.CompilerParams(vmem_limit_bytes=limit),
        cost_estimate=pl.CostEstimate(flops=flops, transcendentals=0, bytes_accessed=0) if flops else None,
    )(*scalars, *inputs)


def request_kernel(rows_held, which, here_ref, hash_ref, *refs):
    *before, out_ref, row_ref, sem = refs
    half = here_ref[0] >> 6

    @pl.when(half == which)
    def _():
        copy = pltpu.make_async_copy(hash_ref, row_ref, sem)
        copy.start()
        copy.wait()
        row = row_ref[...]
        owner = row // rows_held
        local = (row - owner * rows_held).astype(f32)
        owner_rows = jnp.broadcast_to(owner.astype(f32), (LANES, LANES))
        owner_cols = owner_rows.T
        earlier = (owner_rows == owner_cols) & (iota((LANES, LANES), 0) < iota((LANES, LANES), 1))
        slot = jnp.sum(earlier.astype(f32), axis=0, keepdims=True).astype(jnp.int32)
        z = owner >> 5
        near = (z >> 1) == half
        server = (jnp.where(near, z, 3 - z) & 1) * 32 + (owner & 31)
        landing = server * 4 + jnp.where(near, slot, slot + 2)
        rows = out_ref.shape[0]
        place = turn_of(server >> 2) * 16 + (landing & 15)
        asks = jnp.where(place == iota((rows, LANES), 0), local, jnp.zeros((rows, LANES), f32))
        asks = jnp.sum(asks, axis=1, keepdims=True)
        where = landing.astype(f32)
        turned = pltpu.roll(where, LANES // 2, 1)
        first = (iota((rows, LANES), 0) & 3) == 0
        message = jnp.where(iota((rows, LANES), 1) < LANES // 2, asks, jnp.where(first, turned, where))
        out_ref[...] = message.astype(bf16)

    for ref in before:

        @pl.when(half != which)
        def _():
            out_ref[...] = ref[...]


def gather_kernel(asked_ref, mine_ref, other_ref, out_ref):
    index = asked_ref[...].astype(jnp.int32)[:, 0:1]
    rows = index.shape[0]
    held = mine_ref.shape[0]
    index = jnp.where(((iota((rows, 1), 0) >> 1) & 1) == 0, index, index + held)
    chosen = (index == iota((rows, 2 * held), 1)).astype(f32).astype(bf16)
    table = jnp.concatenate([mine_ref[...], other_ref[...]], axis=0)
    found = jnp.dot(chosen, table, preferred_element_type=f32).astype(bf16)
    starts = [turn_of(chip // 2) * 16 for chip in range(rows // 8)]
    both = [found[start : start + 16] for start in starts]
    out_ref[...] = jnp.concatenate(both, axis=0)


def place_kernel(heads, here_ref, asked_ref, arrived_ref, out_ref):
    core = here_ref[0] & 1
    start = pl.multiple_of(turn_of((here_ref[0] >> 2) & 15) * 16, 16)
    asked = asked_ref[pl.ds(start, 16), :].astype(f32)
    arrived = arrived_ref[...]
    slots = arrived.shape[0]
    width = arrived.shape[1]
    low = iota((1, LANES), 1) < LANES // 2
    turned = pltpu.roll(asked, LANES // 2, 1)
    for k, head in enumerate(heads):
        landing = jnp.where(low, turned[4 * head : 4 * head + 1], asked[4 * head + 1 : 4 * head + 2])
        landing = landing.astype(jnp.int32)
        target = (landing >> 3) * 16 + head * 4 + (landing & 3)
        target = jnp.where(((landing >> 2) & 1) == core, target, -1)
        chosen = (target == iota((slots, LANES), 0)).astype(f32).astype(bf16)
        found = lax.dot_general(chosen, arrived, (((0,), (0,)), ((), ())), preferred_element_type=f32)
        out_ref[:, k * width : (k + 1) * width] = found.astype(bf16)


def row_of_sums(terms):
    parts = terms[:, 0:LANES]
    for k in range(1, terms.shape[1] // LANES):
        parts = parts + terms[:, k * LANES : (k + 1) * LANES]
    return jnp.sum(parts.T, axis=0, keepdims=True)


def first_kernel(mine_ref, other_ref, weight_ref, _, out_ref):
    memory = mine_ref[...] + other_ref[...]
    out_ref[...] = jnp.dot(memory, weight_ref[: memory.shape[1], :], preferred_element_type=f32)


def value_kernel(mine0_ref, other0_ref, mine1_ref, other1_ref, weight_ref, out_ref):
    memory = jnp.concatenate([mine0_ref[...] + other0_ref[...], mine1_ref[...] + other1_ref[...]], axis=1)
    out_ref[...] = jnp.dot(memory, weight_ref[...], preferred_element_type=f32)


def key_kernel(mine_ref, other_ref, weight_ref, first_ref, hidden_ref, hgain_ref, kgain_ref, sums_ref):
    memory = mine_ref[...] + other_ref[...]
    key = first_ref[...] + jnp.dot(memory, weight_ref[memory.shape[1] :, :], preferred_element_type=f32)
    hidden = hidden_ref[...].astype(f32)
    sums = [
        row_of_sums(hidden * hidden),
        row_of_sums(key * key),
        row_of_sums((hidden * hgain_ref[...]) * (key * kgain_ref[...])),
    ]
    sums_ref[...] = jnp.concatenate(sums + [jnp.zeros((5, LANES), f32)], axis=0)


def join_kernel(chunks, s0_ref, s1_ref, s2_ref, s3_ref, hidden_ref, projected_ref, out_ref, joined_ref, sems):
    sums = (s0_ref[...] + s1_ref[...]) + (s2_ref[...] + s3_ref[...])
    hidden_power = sums[0:1] / D
    key_power = sums[1:2] / D
    agreement = sums[2:3] * lax.rsqrt(hidden_power + EPSILON) * lax.rsqrt(key_power + EPSILON)
    gate = jax.nn.sigmoid(agreement / math.sqrt(D))
    gate = jnp.broadcast_to(gate, (LANES, LANES)).T
    rows = LANES // chunks
    copies = []
    for k in range(chunks):
        part = slice(k * rows, (k + 1) * rows)
        for column in range(0, joined_ref.shape[1], LANES):
            lanes = slice(column, column + LANES)
            joined = hidden_ref[part, lanes].astype(f32) + gate[part] * projected_ref[part, lanes]
            joined_ref[part, lanes] = joined.astype(bf16)
        copy = pltpu.make_async_copy(joined_ref.at[part, :], out_ref.at[part, :], sems.at[k])
        copy.start()
        copies.append(copy)
    for copy in copies:
        copy.wait()


def local(hidden, hash_rows, memory_table, key_weight, value_weight, hidden_gain, key_gain):
    groups = lax.axis_size("dp")
    tensor = lax.axis_size("tensor")
    devices = groups * tensor
    rows_held, row_width = memory_table.shape
    shape = jax.ShapeDtypeStruct

    here = lax.axis_index(BOTH).astype(jnp.int32).reshape(1)
    hash_rows, here, hidden_gain, key_gain = lax.optimization_barrier((hash_rows, here, hidden_gain, key_gain))
    servers = devices // 2
    rows = pltpu.with_memory_space_constraint(hash_rows.reshape(1, LANES), pltpu.HBM)

    def request(which, *before):
        return pl.pallas_call(
            lambda *refs: request_kernel(rows_held, which, *refs),
            out_shape=shape((4 * servers, LANES), bf16),
            in_specs=[pl.BlockSpec(memory_space=pltpu.SMEM), pl.BlockSpec(memory_space=pltpu.HBM)] + vmem(len(before)),
            out_specs=vmem(1)[0],
            scratch_shapes=[pltpu.VMEM((1, LANES), jnp.int32), pltpu.SemaphoreType.DMA(())],
            compiler_params=pltpu.CompilerParams(vmem_limit_bytes=2 * MIB),
            cost_estimate=pl.CostEstimate(flops=COVER if before else 1, transcendentals=0, bytes_accessed=1),
        )(here, rows, *before)

    message = request(0)
    message, memory_table = lax.optimization_barrier((message, memory_table))
    swap = [(k, (3 - (k >> 5)) * 32 + (k & 31)) for k in range(devices)]
    table_there = lax.ppermute(memory_table, BOTH, swap)
    message = request(1, message)
    halves_of_z = [[half * servers + k for k in range(servers)] for half in range(2)]
    same_core = [[k for k in half if k % 2 == core] for half in halves_of_z for core in range(2)]
    by_group = [[half[4 * group + k] for group in group_order() for k in range(4)] for half in halves_of_z]
    asked = lax.all_to_all(
        message.reshape(servers, 4, LANES), BOTH, 0, 0, axis_index_groups=by_group, tiled=True
    ).reshape(4 * servers, LANES)
    sent = call(
        gather_kernel,
        shape((8 * servers, row_width), bf16),
        [asked, memory_table, table_there],
        6 * MIB,
        flops=COVER // 2,
    )
    arrived = lax.all_to_all(
        sent.reshape(servers // 2, 16, row_width), BOTH, 0, 0, axis_index_groups=same_core, tiled=True
    ).reshape(8 * servers, row_width)
    halves = []
    for heads in ((0, 1), (2, 3)):
        mine = call(
            lambda *refs, heads=heads: place_kernel(heads, *refs),
            shape((LANES, 2 * row_width), bf16),
            [asked, arrived],
            6 * MIB,
            scalars=[here],
        )
        halves.append((mine, lax.ppermute(mine, "tensor", [(k, k ^ 1) for k in range(tensor)])))
    columns = key_weight.shape[1]
    work = 2 * LANES * 2 * row_width * columns
    key_weight = pltpu.with_memory_space_constraint(key_weight, pltpu.VMEM)
    value_weight = pltpu.with_memory_space_constraint(value_weight, pltpu.VMEM)
    partial = shape((LANES, columns), f32)
    key = call(first_kernel, partial, [*halves[0], key_weight, value_weight], 6 * MIB, flops=work)
    sums = call(
        key_kernel,
        shape((8, LANES), f32),
        [*halves[1], key_weight, key, hidden, hidden_gain.reshape(1, columns), key_gain.reshape(1, columns)],
        6 * MIB,
        flops=work,
    )
    others = [lax.ppermute(sums, "tensor", [(k, k ^ d) for k in range(tensor)]) for d in (2, 3, 1)]
    projected = call(value_kernel, partial, [*halves[0], *halves[1], value_weight], 6 * MIB, flops=2 * work)
    chunks = 2
    return pl.pallas_call(
        lambda *refs: join_kernel(chunks, *refs),
        out_shape=shape(hidden.shape, bf16),
        in_specs=vmem(6),
        out_specs=pl.BlockSpec(memory_space=pl.ANY),
        scratch_shapes=[pltpu.VMEM(hidden.shape, bf16), pltpu.SemaphoreType.DMA((chunks,))],
        compiler_params=pltpu.CompilerParams(vmem_limit_bytes=6 * MIB),
    )(sums, *others, hidden, projected)


def solution(mesh):
    return jax.shard_map(
        local,
        mesh=mesh,
        in_specs=(
            P("dp", "tensor"),
            P("dp", "tensor"),
            P(("dp", "tensor"), None),
            P(None, "tensor"),
            P(None, "tensor"),
            P("tensor"),
            P("tensor"),
        ),
        out_specs=P("dp", "tensor"),
        check_vma=False,
    )
```
